8 devices in a mesh: dp: 2 (over z, y), sp: 4 (over x, core).
Axes of the slice: x: 2, y: 2, z: 1, core: 2. Of those that a mesh axis runs over, the one named last changes fastest.
Arguments:
- x_in: bfloat16 [32, 1024, 2048], P('dp', 'sp'), parts along dimension 0
- grad_y: bfloat16 [32, 1024, 2048], P('dp', 'sp'), parts along dimension 0
- positions: int32 [32, 1024], P('dp', 'sp'), parts along dimension 0
- g_norm: bfloat16 [2048], replicated
- w_query: bfloat16 [2048, 2048], replicated
- w_key: bfloat16 [2048, 2048], replicated
- w_value: bfloat16 [2048, 2048], replicated
- w_out: bfloat16 [2048, 2048], replicated
- g_query: bfloat16 [2048], replicated
- g_key: bfloat16 [2048], replicated
Outputs:
- output 1: bfloat16 [32, 1024, 2048], P('dp', 'sp'), parts along dimension 0
- output 2: bfloat16 [32, 1024, 2048], P('dp', 'sp'), parts along dimension 0
- output 3: float32 [4096], P(('dp', 'sp')), parts along dimension 0
- output 4: float32 [4096, 2048], P(('dp', 'sp')), parts along dimension 0
- output 5: float32 [4096, 2048], P(('dp', 'sp')), parts along dimension 0
- output 6: float32 [4096, 2048], P(('dp', 'sp')), parts along dimension 0
- output 7: float32 [4096, 2048], P(('dp', 'sp')), parts along dimension 0
- output 8: float32 [4096], P(('dp', 'sp')), parts along dimension 0
- output 9: float32 [4096], P(('dp', 'sp')), parts along dimension 0
There are 2 independent parts. The reference program is written for one: setup_inputs(seed, part) draws one part's arguments, and reference() takes and returns one part's arrays. A program takes and returns all parts, laid end to end along the dimension named above; an argument that names none is the same for every part.
All inputs are finite; a program needn't handle non-finite values.
Results may differ from the reference program's by a relative error of at most 0.0114701.
Values are sent between devices in bfloat16 or wider.
A program may use at most 1 GiB of HBM per device.

```python
import jax
import jax.numpy as jnp
from jax import lax

N_BATCH = 16
SEQ_LEN = 1024
D_MODEL = 2048
N_HEADS = 16
HEAD_DIM = 128
QUERY_BLOCK = min(128, SEQ_LEN)
NORM_EPS = 1e-5
ROPE_BASE = 10000.0
NEG_BIG = -1e30


def setup_inputs(seed: int = 0, part: int = 0) -> dict:
    part_key = jax.random.fold_in(jax.random.key(seed), part)
    key_x, key_dy, key_pos = jax.random.split(part_key, 3)
    weight_keys = jax.random.split(jax.random.key(seed + 1), 9)
    act_shape = (N_BATCH, SEQ_LEN, D_MODEL)
    x_in = jax.random.normal(key_x, act_shape, jnp.float32).astype(jnp.bfloat16)
    grad_y = jax.random.normal(key_dy, act_shape, jnp.float32).astype(jnp.bfloat16)
    tok_idx = jnp.arange(SEQ_LEN, dtype=jnp.int32)
    restart = jax.random.randint(key_pos, (N_BATCH, SEQ_LEN), 0, 256) == 0
    doc_start = lax.cummax(jnp.where(restart, tok_idx[None, :], 0), axis=1)
    positions = (tok_idx[None, :] - doc_start).astype(jnp.int32)
    fan_scale = D_MODEL ** -0.5
    head_q = jnp.repeat(jax.random.uniform(weight_keys[0], (N_HEADS,), jnp.float32, 0.5, 1.5), HEAD_DIM)
    head_k = jnp.repeat(jax.random.uniform(weight_keys[1], (N_HEADS,), jnp.float32, 0.5, 1.5), HEAD_DIM)
    w_shape = (D_MODEL, D_MODEL)
    w_query = (jax.random.normal(weight_keys[2], w_shape, jnp.float32) * fan_scale * head_q[None, :]).astype(jnp.bfloat16)
    w_key = (jax.random.normal(weight_keys[3], w_shape, jnp.float32) * fan_scale * head_k[None, :]).astype(jnp.bfloat16)
    w_value = (jax.random.normal(weight_keys[4], w_shape, jnp.float32) * fan_scale).astype(jnp.bfloat16)
    w_out = (jax.random.normal(weight_keys[5], w_shape, jnp.float32) * fan_scale).astype(jnp.bfloat16)
    g_norm = (1.0 + 0.3 * jax.random.normal(weight_keys[6], (D_MODEL,), jnp.float32)).astype(jnp.bfloat16)
    g_query = (1.7 + 0.4 * jax.random.normal(weight_keys[7], (D_MODEL,), jnp.float32)).astype(jnp.bfloat16)
    g_key = (1.7 + 0.4 * jax.random.normal(weight_keys[8], (D_MODEL,), jnp.float32)).astype(jnp.bfloat16)
    return {'x_in': x_in, 'grad_y': grad_y, 'positions': positions, 'g_norm': g_norm, 'w_query': w_query, 'w_key': w_key, 'w_value': w_value, 'w_out': w_out, 'g_query': g_query, 'g_key': g_key}


def rms_scale(values, gain_vec):
    inv_rms = lax.rsqrt(jnp.mean(values * values, axis=-1, keepdims=True) + NORM_EPS)
    return values * inv_rms * gain_vec


def rope_tables(positions):
    half_dim = HEAD_DIM // 2
    inv_freq = ROPE_BASE ** (-jnp.arange(half_dim, dtype=jnp.float32) * (2.0 / HEAD_DIM))
    angles = positions.astype(jnp.float32)[..., None] * inv_freq
    return jnp.cos(angles)[:, :, None, :], jnp.sin(angles)[:, :, None, :]


def rope_apply(values, cos_t, sin_t):
    half_dim = values.shape[-1] // 2
    first_half = values[..., :half_dim]
    second_half = values[..., half_dim:]
    return jnp.concatenate([first_half * cos_t - second_half * sin_t, second_half * cos_t + first_half * sin_t], axis=-1)


def mat_f32(left_op, right_op):
    return jnp.dot(left_op, right_op, precision=lax.Precision.HIGHEST)


def causal_attention(q_bf, k_bf, v_bf):
    q_f = q_bf.astype(jnp.float32)
    k_f = k_bf.astype(jnp.float32)
    v_f = v_bf.astype(jnp.float32)
    key_pos = jnp.arange(SEQ_LEN)
    qk_scale = HEAD_DIM ** -0.5

    def one_block(q_start):
        q_blk = lax.dynamic_slice_in_dim(q_f, q_start, QUERY_BLOCK, axis=1)
        scores = jnp.einsum('bqhd,bkhd->bhqk', q_blk, k_f, precision=lax.Precision.HIGHEST) * qk_scale
        q_pos = q_start + jnp.arange(QUERY_BLOCK)
        scores = jnp.where(q_pos[:, None] >= key_pos[None, :], scores, NEG_BIG)
        prob_f = jax.nn.softmax(scores, axis=-1)
        return jnp.einsum('bhqk,bkhd->bqhd', prob_f, v_f, precision=lax.Precision.HIGHEST)

    starts = jnp.arange(SEQ_LEN // QUERY_BLOCK) * QUERY_BLOCK
    blocks = lax.map(jax.checkpoint(one_block), starts)
    merged = jnp.moveaxis(blocks, 0, 1).reshape(q_bf.shape)
    return merged.astype(jnp.bfloat16)


def reference(x_in, grad_y, positions, g_norm, w_query, w_key, w_value, w_out, g_query, g_key):
    cos_t, sin_t = rope_tables(positions)
    head_shape = (N_BATCH, SEQ_LEN, N_HEADS, HEAD_DIM)
    flat_shape = (N_BATCH, SEQ_LEN, D_MODEL)

    def forward(x_f, gain_n, wq_f, wk_f, wv_f, wo_f, gain_q, gain_k):
        hidden = rms_scale(x_f, gain_n).astype(jnp.bfloat16).astype(jnp.float32)
        q_raw = mat_f32(hidden, wq_f)
        k_raw = mat_f32(hidden, wk_f)
        v_val = mat_f32(hidden, wv_f).astype(jnp.bfloat16)
        q_rot = rope_apply(rms_scale(q_raw, gain_q).reshape(head_shape), cos_t, sin_t).astype(jnp.bfloat16)
        k_rot = rope_apply(rms_scale(k_raw, gain_k).reshape(head_shape), cos_t, sin_t).astype(jnp.bfloat16)
        attended = causal_attention(q_rot, k_rot, v_val.reshape(head_shape))
        o_proj = mat_f32(attended.reshape(flat_shape).astype(jnp.float32), wo_f)
        return (x_f + o_proj).astype(jnp.bfloat16)

    y_out, pullback = jax.vjp(forward, x_in.astype(jnp.float32), g_norm.astype(jnp.float32), w_query.astype(jnp.float32), w_key.astype(jnp.float32), w_value.astype(jnp.float32), w_out.astype(jnp.float32), g_query.astype(jnp.float32), g_key.astype(jnp.float32))
    cotangents = pullback(grad_y)
    return (y_out, cotangents[0].astype(jnp.bfloat16), cotangents[1], cotangents[2], cotangents[3], cotangents[4], cotangents[5], cotangents[6], cotangents[7])
```

```python
import math
import jax
import jax.numpy as jnp
from jax import lax
from jax.experimental import pallas as pl
from jax.experimental.pallas import tpu as pltpu
from jax.sharding import PartitionSpec as P


HEAD = 128
EPS = 1e-5
ROPE_BASE = 10000.0
NEG_BIG = -1e30
SCALE = HEAD ** -0.5
SCALE2 = SCALE * math.log2(math.e)
N_CHUNK = 2
VMEM = 66_000_000
F32 = jnp.float32
BF16 = jnp.bfloat16


def dot_nn(a, b):
    return lax.dot_general(a, b, (((1,), (0,)), ((), ())), preferred_element_type=F32)


def dot_nt(a, b):
    return lax.dot_general(a, b, (((1,), (1,)), ((), ())), preferred_element_type=F32)


def dot_tn(a, b):
    return lax.dot_general(a, b, (((0,), (0,)), ((), ())), preferred_element_type=F32)


def head_cols(idx):
    return slice(idx * HEAD, (idx + 1) * HEAD)


def row_sum(part):
    return jnp.sum(part, axis=-1, keepdims=True)


ANY = pl.BlockSpec(memory_space=pl.ANY)


def place(bits):
    return jnp.where((bits == 0) | (bits == 3), 3 - bits, bits)


def front_kernel(me_ref, xa_ref, xb_ref, cos_ref, sin_ref, gn_ref, gq_ref, gk_ref, wq_ref, wk_ref, wv_ref, *refs):
    x_ref, h_ref, q_ref, k_ref, v_ref, q1_ref, k1_ref = refs[-7:]
    d_model = x_ref.shape[-1]
    n_heads = d_model // HEAD

    @pl.when(pl.program_id(0) == 0)
    def _():
        x_ref[...] = xa_ref[...]

    @pl.when(pl.program_id(0) == 1)
    def _():
        x_ref[...] = xb_ref[...]

    x_f = x_ref[...].astype(F32)
    inv_x = lax.rsqrt(jnp.mean(x_f * x_f, axis=-1, keepdims=True) + EPS)
    hidden = (x_f * inv_x * gn_ref[...]).astype(BF16)
    blk = d_model // 4
    for b in range(4):
        h_ref[:, pl.ds(pl.multiple_of(place(me_ref[0] ^ b) * blk, blk), blk)] = hidden[:, b * blk:(b + 1) * blk]
    cos_t = cos_ref[...]
    sin_t = sin_ref[...]
    n_col = 512
    for w_ref, g_ref, raw_ref, out_ref in ((wq_ref, gq_ref, q1_ref, q_ref), (wk_ref, gk_ref, k1_ref, k_ref)):
        sq = jnp.zeros((x_ref.shape[0], HEAD), F32)
        for c0 in range(0, d_model, n_col):
            raw = dot_nn(hidden, w_ref[:, c0:c0 + n_col])
            raw_ref[:, c0:c0 + n_col] = raw
            for j in range(n_col // HEAD):
                piece = raw[:, head_cols(j)]
                sq = sq + piece * piece
        inv = lax.rsqrt(row_sum(sq) * (1.0 / d_model) + EPS)
        for j in range(n_heads):
            u = raw_ref[:, head_cols(j)] * inv * g_ref[:, head_cols(j)]
            rot = u * cos_t + pltpu.roll(u, HEAD // 2, 1) * sin_t
            out_ref[:, head_cols(j)] = rot.astype(BF16)
    for c0 in range(0, d_model, n_col):
        v_ref[:, c0:c0 + n_col] = dot_nn(hidden, wv_ref[:, c0:c0 + n_col]).astype(BF16)


def front(me, x_a, x_b, own, bits, seq0, n_seq, cos_t, sin_t, g_norm, g_query, g_key, w_query, w_key, w_value, filled):
    n_piece, n_all, rows, d_model = cos_t.shape[:3] + x_a.shape[-1:]
    first = lambda i, s: jnp.where(i == 0, s, n_seq - 1)
    second = lambda i, s: jnp.where(i == 0, 0, s)
    x_block = (None, rows, d_model)
    a_map = (lambda i, s, m: (m[0] * n_all + first(i, s), 0, 0)) if own else (lambda i, s, m: (first(i, s), 0, 0))
    spot = lambda i, s, m: (m[0] ^ jnp.where(i == 0, bits[0], bits[1]), seq0 + s, 0, 0)
    table = pl.BlockSpec((None, None, rows, HEAD), spot)
    out = pl.BlockSpec((None, None, rows, d_model), spot)
    vec = pl.BlockSpec((1, d_model), lambda i, s, m: (0, 0))
    mat = pl.BlockSpec((d_model, d_model), lambda i, s, m: (0, 0), pipeline_mode=pl.Buffered(1))
    big = lambda dt: jax.ShapeDtypeStruct((n_piece, n_all, rows, d_model), dt)
    row = lambda g: g.astype(F32).reshape(1, d_model)
    n_tok = 2 * n_seq * rows
    return pl.pallas_call(
        front_kernel,
        grid_spec=pltpu.PrefetchScalarGridSpec(
            num_scalar_prefetch=1,
            grid=(2, n_seq),
            in_specs=[pl.BlockSpec(x_block, a_map), pl.BlockSpec(x_block, lambda i, s, m: (second(i, s), 0, 0)), table, table, vec, vec, vec, mat, mat, mat] + [ANY] * len(filled),
            out_specs=[out] * 7,
        ),
        out_shape=[big(BF16)] * 5 + [big(F32)] * 2,
        input_output_aliases={11 + n: n for n in range(len(filled))},
        compiler_params=pltpu.CompilerParams(vmem_limit_bytes=VMEM, dimension_semantics=("arbitrary", "arbitrary")),
        cost_estimate=pl.CostEstimate(flops=6 * n_tok * d_model * d_model, bytes_accessed=n_tok * d_model * 20 + 6 * d_model * d_model, transcendentals=0),
        name="front",
    )(me, x_a, x_b, cos_t, sin_t, row(g_norm), row(g_query), row(g_key), w_query, w_key, w_value, *filled)


def attend_kernel(me_ref, q_ref, k_ref, v_ref, *refs):
    o_ref, rel_ref, lse_ref = refs[-3:]
    n_piece, _, rows, width = q_ref.shape
    keep = lax.broadcasted_iota(jnp.int32, (rows, rows), 0) >= lax.broadcasted_iota(jnp.int32, (rows, rows), 1)
    for hd in range(width // HEAD):
        cols = head_cols(hd)
        for i in range(n_piece):
            q_i = q_ref[i, 0, :, cols]
            scores = [dot_nt(q_i, k_ref[j, 0, :, cols]) for j in range(i + 1)]
            scores[i] = jnp.where(keep, scores[i], NEG_BIG)
            top = scores[0]
            for j in range(1, i + 1):
                top = jnp.maximum(top, scores[j])
            top = jnp.max(top, axis=-1, keepdims=True) * SCALE2
            total = None
            out = None
            for j in range(i + 1):
                prob = jnp.exp2(scores[j] * SCALE2 - top)
                total = prob if total is None else total + prob
                term = dot_nn(prob.astype(BF16), v_ref[j, 0, :, cols])
                out = term if out is None else out + term
            total = row_sum(total)
            out = (out * (1.0 / total)).astype(BF16)
            o_ref[i, 0, :, cols] = out
            rel_ref[i, 0, :, cols] = out
            lse = top + jnp.log2(total)
            lse_ref[0, hd, :, i * rows:(i + 1) * rows] = jnp.broadcast_to(lse, (rows, HEAD)).T[0:1, :]


def attend(me, q_all, k_all, v_all, seq0, n_seq, filled, heads=2):
    n_piece, n_all, rows, d_model = q_all.shape
    n_heads = d_model // HEAD
    per = n_heads // heads // 4
    shape = (n_piece, 1, rows, heads * HEAD)
    blk = pl.BlockSpec(shape, lambda s, h, m: (0, seq0 + s, 0, h))
    rel = pl.BlockSpec(shape, lambda s, h, m: (0, seq0 + s, 0, place(m[0] ^ (h // per)) * per + h % per))
    seq = n_piece * rows
    big = jax.ShapeDtypeStruct(q_all.shape, BF16)
    return pl.pallas_call(
        attend_kernel,
        grid_spec=pltpu.PrefetchScalarGridSpec(
            num_scalar_prefetch=1,
            grid=(n_seq, n_heads // heads),
            in_specs=[blk] * 3 + [ANY] * len(filled),
            out_specs=[blk, rel, pl.BlockSpec((1, heads, 1, seq), lambda s, h, m: (seq0 + s, h, 0, 0))],
        ),
        out_shape=[big, big, jax.ShapeDtypeStruct((n_all, n_heads, 1, seq), F32)],
        input_output_aliases={4 + n: n for n in range(len(filled))},
        compiler_params=pltpu.CompilerParams(vmem_limit_bytes=VMEM, dimension_semantics=("arbitrary", "arbitrary")),
        cost_estimate=pl.CostEstimate(flops=6 * n_seq * seq * seq * d_model, bytes_accessed=10 * n_seq * seq * d_model, transcendentals=0),
        name="attend",
    )(me, q_all, k_all, v_all, *filled)


def attend_back_kernel(q_ref, k_ref, v_ref, do_ref, lse_ref, dq_ref, dk_ref, dv_ref, dk_acc, dv_acc):
    n_piece, _, rows, width = q_ref.shape
    keep = lax.broadcasted_iota(jnp.int32, (rows, rows), 0) <= lax.broadcasted_iota(jnp.int32, (rows, rows), 1)
    for hd in range(width // HEAD):
        cols = head_cols(hd)
        k_t = [k_ref[j, 0, :, cols].T for j in range(n_piece)]
        for i in range(n_piece):
            q_i = q_ref[i, 0, :, cols]
            do_i = do_ref[i, 0, :, cols]
            lse = lse_ref[0, hd, :, i * rows:(i + 1) * rows]
            probs, d_probs = [], []
            row_dot = None
            for j in range(i + 1):
                prob = jnp.exp2(dot_nt(k_ref[j, 0, :, cols], q_i) * SCALE2 - lse)
                if j == i:
                    prob = jnp.where(keep, prob, 0.0)
                d_prob = dot_nt(v_ref[j, 0, :, cols], do_i)
                part = jnp.sum(prob * d_prob, axis=0, keepdims=True)
                row_dot = part if row_dot is None else row_dot + part
                probs.append(prob)
                d_probs.append(d_prob)
            dq_t = None
            for j in range(i + 1):
                d_s = (probs[j] * (d_probs[j] - row_dot) * SCALE).astype(BF16)
                dv_term = dot_nn(probs[j].astype(BF16), do_i)
                dk_term = dot_nn(d_s, q_i)
                dq_term = dot_nn(k_t[j], d_s)
                dq_t = dq_term if dq_t is None else dq_t + dq_term
                if i == j:
                    dv_acc[hd, j] = dv_term
                    dk_acc[hd, j] = dk_term
                else:
                    dv_acc[hd, j] += dv_term
                    dk_acc[hd, j] += dk_term
            dq_ref[i, 0, :, cols] = dq_t.T.astype(BF16)
        for j in range(n_piece):
            dk_ref[j, 0, :, cols] = dk_acc[hd, j].astype(BF16)
            dv_ref[j, 0, :, cols] = dv_acc[hd, j].astype(BF16)


def attend_back(q_all, k_all, v_all, d_out, lse, heads=2):
    n_piece, n_seq, rows, d_model = q_all.shape
    n_heads = d_model // HEAD
    blk = pl.BlockSpec((n_piece, 1, rows, heads * HEAD), lambda s, h: (0, s, 0, h))
    seq = n_piece * rows
    return pl.pallas_call(
        attend_back_kernel,
        grid=(n_seq, n_heads // heads),
        in_specs=[blk] * 4 + [pl.BlockSpec((1, heads, 1, seq), lambda s, h: (s, h, 0, 0))],
        out_specs=[blk] * 3,
        out_shape=[jax.ShapeDtypeStruct(q_all.shape, BF16)] * 3,
        scratch_shapes=[pltpu.VMEM((heads, n_piece, rows, HEAD), F32)] * 2,
        compiler_params=pltpu.CompilerParams(vmem_limit_bytes=VMEM, dimension_semantics=("arbitrary", "arbitrary")),
        cost_estimate=pl.CostEstimate(flops=14 * n_seq * seq * seq * d_model, bytes_accessed=14 * n_seq * seq * d_model, transcendentals=0),
        name="attend_back",
    )(q_all, k_all, v_all, d_out, lse)


def tail_kernel(dq_ref, dk_ref, dv_ref, q1_ref, k1_ref, x_ref, dy_ref, cos_ref, sin_ref, gn_ref, gq_ref, gk_ref, wq_ref, wk_ref, wv_ref, *refs):
    dqr_ref, dkr_ref, gx_ref, ggn_ref, ggq_ref, ggk_ref, dh_ref, rot_ref = refs[-8:]
    rows, d_model = x_ref.shape
    n_heads = d_model // HEAD
    n_col = 512
    cos_t = cos_ref[...]
    sin_t = sin_ref[...]

    @pl.when((pl.program_id(0) == 0) & (pl.program_id(1) == 0))
    def _():
        for ref in (ggn_ref, ggq_ref, ggk_ref):
            ref[...] = jnp.zeros_like(ref)

    dv_b = dv_ref[...]
    for c0 in range(0, d_model, n_col):
        dh_ref[:, c0:c0 + n_col] = dot_nt(dv_b, wv_ref[c0:c0 + n_col, :])
    for d_ref, raw_ref, g_ref, w_ref, dr_ref, gg_ref in ((dq_ref, q1_ref, gq_ref, wq_ref, dqr_ref, ggq_ref), (dk_ref, k1_ref, gk_ref, wk_ref, dkr_ref, ggk_ref)):
        sq = jnp.zeros((rows, HEAD), F32)
        cross = jnp.zeros((rows, HEAD), F32)
        for j in range(n_heads):
            u = raw_ref[:, head_cols(j)]
            d = d_ref[:, head_cols(j)].astype(F32)
            d = d * cos_t - pltpu.roll(d, HEAD // 2, 1) * sin_t
            rot_ref[:, head_cols(j)] = d
            sq = sq + u * u
            cross = cross + d * g_ref[:, head_cols(j)] * u
        inv = lax.rsqrt(row_sum(sq) * (1.0 / d_model) + EPS)
        coef = row_sum(cross) * (1.0 / d_model) * inv * inv
        for j in range(n_heads):
            u = raw_ref[:, head_cols(j)]
            d = rot_ref[:, head_cols(j)]
            gg_ref[:, head_cols(j)] += jnp.sum(d * (u * inv), axis=0, keepdims=True)
            dr_ref[:, head_cols(j)] = (inv * (d * g_ref[:, head_cols(j)] - u * coef)).astype(BF16)
        d_b = dr_ref[...]
        for c0 in range(0, d_model, n_col):
            dh_ref[:, c0:c0 + n_col] += dot_nt(d_b, w_ref[c0:c0 + n_col, :])
    sq = jnp.zeros((rows, HEAD), F32)
    cross = jnp.zeros((rows, HEAD), F32)
    for j in range(n_heads):
        u = x_ref[:, head_cols(j)].astype(F32)
        sq = sq + u * u
        cross = cross + dh_ref[:, head_cols(j)] * gn_ref[:, head_cols(j)] * u
    inv = lax.rsqrt(row_sum(sq) * (1.0 / d_model) + EPS)
    coef = row_sum(cross) * (1.0 / d_model) * inv * inv
    for j in range(n_heads):
        u = x_ref[:, head_cols(j)].astype(F32)
        d = dh_ref[:, head_cols(j)]
        ggn_ref[:, head_cols(j)] += jnp.sum(d * (u * inv), axis=0, keepdims=True)
        g_x = dy_ref[:, head_cols(j)].astype(F32) + inv * (d * gn_ref[:, head_cols(j)] - u * coef)
        gx_ref[:, head_cols(j)] = g_x.astype(BF16)


def tail(dq, dk, dv, q1, k1, x_all, dy_all, cos_t, sin_t, g_norm, g_query, g_key, w_query, w_key, w_value, seq0, n_seq, filled):
    n_piece, _, rows, d_model = x_all.shape
    spot = lambda i, s: (i, seq0 + s, 0, 0)
    tok = pl.BlockSpec((None, None, rows, d_model), spot)
    table = pl.BlockSpec((None, None, rows, HEAD), spot)
    vec = pl.BlockSpec((1, d_model), lambda i, s: (0, 0))
    mat = pl.BlockSpec((d_model, d_model), lambda i, s: (0, 0), pipeline_mode=pl.Buffered(1))
    big = jax.ShapeDtypeStruct(x_all.shape, BF16)
    small = jax.ShapeDtypeStruct((1, d_model), F32)
    row = lambda g: g.astype(F32).reshape(1, d_model)
    n_tok = n_piece * n_seq * rows
    return pl.pallas_call(
        tail_kernel,
        grid=(n_piece, n_seq),
        in_specs=[tok] * 7 + [table] * 2 + [vec] * 3 + [mat] * 3 + [ANY] * len(filled),
        out_specs=[tok] * 3 + [vec] * 3,
        out_shape=[big] * 3 + [small] * 3,
        input_output_aliases={15 + n: n for n in range(len(filled))},
        scratch_shapes=[pltpu.VMEM((rows, d_model), F32)] * 2,
        compiler_params=pltpu.CompilerParams(vmem_limit_bytes=VMEM, dimension_semantics=("arbitrary", "arbitrary")),
        cost_estimate=pl.CostEstimate(flops=6 * n_tok * d_model * d_model, bytes_accessed=n_tok * d_model * 24 + 6 * d_model * d_model, transcendentals=0),
        name="tail",
    )(dq, dk, dv, q1, k1, x_all, dy_all, cos_t, sin_t, row(g_norm), row(g_query), row(g_key), w_query, w_key, w_value, *filled)


def rope_tables(positions):
    half = HEAD // 2
    inv_freq = ROPE_BASE ** (-jnp.arange(half, dtype=F32) * (2.0 / HEAD))
    angles = positions.astype(F32)[..., None] * inv_freq
    cos_t = jnp.cos(angles)
    sin_t = jnp.sin(angles)
    return jnp.concatenate([cos_t, cos_t], axis=-1), jnp.concatenate([-sin_t, sin_t], axis=-1)


def after(value, *earlier):
    return lax.optimization_barrier((value,) + earlier)[0]


def solution(mesh):
    n_sp = mesh.shape['sp']

    def to_peer(value, bits):
        return lax.ppermute(value, 'sp', [(i, i ^ bits) for i in range(n_sp)])

    def device_step(x_loc, grad_y, positions, g_norm, w_query, w_key, w_value, w_out, g_query, g_key):
        n_batch, rows, d_model = x_loc.shape
        n_seq = n_batch // n_sp
        step = n_seq // N_CHUNK
        me = lax.axis_index('sp')
        me_vec = jnp.reshape(me, (1,)).astype(jnp.int32)
        shape4 = (n_sp, n_seq, rows, d_model)
        flat = lambda arr: arr.reshape(-1, d_model)
        far_bits = (2, 3, 1)

        def piece(arr, bits, seq0, count):
            return lax.dynamic_slice(arr, (me ^ bits, seq0, 0, 0), (1, count, rows, d_model))

        def pieces(arr, seq0, count):
            cut = lax.optimization_barrier((arr,) + tuple(piece(arr, bits, seq0, count) for bits in far_bits))
            return cut[0], cut[1:]

        def send(parts):
            return [to_peer(p, bits) for p, bits in zip(parts, far_bits)]

        def put(buf, got, bits, seq0):
            return lax.dynamic_update_slice(buf, got, (me ^ bits, seq0, 0, 0))

        def grad_rows(rel, right):
            half = d_model // 2
            out = to_peer(dot_tn(rel[:, :half], right), 1)
            keep = dot_tn(rel[:, half:], right)
            far = keep[:half // 2] + out[:half // 2]
            got = to_peer(far, 2)
            return (keep[half // 2:], out[half // 2:], got), far

        pos = lax.all_to_all(positions.reshape(n_sp, n_seq, rows), 'sp', split_axis=0, concat_axis=0, tiled=True)
        x4 = x_loc.reshape(shape4)
        x_parts = [piece(x4, 1, 0, n_seq)[0]] + [piece(x4, bits, c * step, step)[0] for c in range(N_CHUNK) for bits in (2, 3)]
        x_near = to_peer(x_parts[0], 1)
        x_far = [[to_peer(x_parts[2 * c + bits - 1], bits) for bits in (2, 3)] for c in range(N_CHUNK)]
        dy4 = after(grad_y.reshape(shape4), *x_parts)
        dy4, dy_parts = pieces(dy4, 0, n_seq)
        dy_got = send(dy_parts)
        cos_t, sin_t = rope_tables(pos)
        gains_in = (g_norm, g_query, g_key)
        weights = (w_query, w_key, w_value)
        filled = front(me_vec, x_loc, x_near, True, (0, 1), 0, n_seq, cos_t, sin_t, *gains_in, *weights, ())
        attn = ()
        prev = cos_t
        for c in range(N_CHUNK):
            filled = front(me_vec, x_far[c][0], x_far[c][1], False, (2, 3), c * step, step, after(cos_t, prev), sin_t, *gains_in, *weights, tuple(filled))
            attn = attend(me_vec, filled[2], filled[3], filled[4], c * step, step, tuple(attn))
            prev = attn[2]
        x_all, h_rel, q, k, v, q1, k1 = filled
        attn, attn_rel, lse = attn
        y = (flat(x_all).astype(F32) + dot_nn(flat(attn), w_out)).astype(BF16).reshape(shape4)
        y, y_parts = pieces(y, 0, n_seq)
        y_got = send(y_parts)
        dy_all = jnp.where(after(me, *x_parts) >= 0, dy4, jnp.zeros_like(dy4))
        for bits, got in zip(far_bits, dy_got):
            dy_all = put(dy_all, after(got, y), bits, 0)
        w_o, far_o = grad_rows(flat(attn_rel), flat(dy_all))
        d_attn = dot_nt(flat(dy_all), w_out).astype(BF16).reshape(shape4)
        dq, dk, dv = attend_back(q, k, v, d_attn, after(lse, far_o))
        w_v, prev = grad_rows(flat(h_rel), flat(dv))
        tails = ()
        gains = 0.0
        gx_got = []
        for c in range(N_CHUNK):
            *tails, ggn, ggq, ggk = tail(dq, dk, dv, q1, k1, x_all, dy_all, after(cos_t, prev), sin_t, *gains_in, *weights, c * step, step, tuple(tails))
            tails[2], gx_parts = pieces(tails[2], c * step, step)
            gx_got.append(send(gx_parts))
            prev = gx_parts[0]
            gains = gains + jnp.concatenate([ggn, ggq, ggk], axis=0)
        dqr, dkr, gx = tails
        w_q, prev = grad_rows(flat(h_rel), flat(after(dqr, prev)))
        w_k, prev = grad_rows(flat(h_rel), flat(after(dkr, prev)))
        for bits, got in zip(far_bits, y_got):
            y = put(y, got, bits, 0)
        for c in range(N_CHUNK):
            for bits, got in zip(far_bits, gx_got[c]):
                gx = put(gx, got, bits, c * step)
        gains = gains + to_peer(gains, 1)
        gains = gains + to_peer(gains, 2)
        gains = lax.dynamic_slice_in_dim(gains, me * (d_model // n_sp), d_model // n_sp, axis=1)
        total = lambda terms: terms[0] + terms[1] + terms[2]
        join = lambda arr: arr.reshape(x_loc.shape)
        return (join(y), join(gx), gains[0], total(w_q), total(w_k), total(w_v), total(w_o), gains[1], gains[2])

    seq_spec = P('dp', 'sp', None)
    mat_rep = P(None, None)
    vec_rep = P(None)
    row_spec = P(('dp', 'sp'), None)
    vec_spec = P(('dp', 'sp'))
    return jax.shard_map(device_step, mesh=mesh, in_specs=(seq_spec, seq_spec, P('dp', 'sp'), vec_rep, mat_rep, mat_rep, mat_rep, mat_rep, vec_rep, vec_rep), out_specs=(seq_spec, seq_spec, vec_spec, row_spec, row_spec, row_spec, row_spec, vec_spec, vec_spec), check_vma=False)
```

```python
import math
import jax
import jax.numpy as jnp
from jax import lax
from jax.experimental import pallas as pl
from jax.experimental.pallas import tpu as pltpu
from jax.sharding import PartitionSpec as P


HEAD = 128
EPS = 1e-5
ROPE_BASE = 10000.0
NEG_BIG = -1e30
SCALE = HEAD ** -0.5
SCALE2 = SCALE * math.log2(math.e)
N_CHUNK = 2
VMEM = 66_000_000
F32 = jnp.float32
BF16 = jnp.bfloat16


def dot_nn(a, b):
    return lax.dot_general(a, b, (((1,), (0,)), ((), ())), preferred_element_type=F32)


def dot_nt(a, b):
    return lax.dot_general(a, b, (((1,), (1,)), ((), ())), preferred_element_type=F32)


def dot_tn(a, b):
    return lax.dot_general(a, b, (((0,), (0,)), ((), ())), preferred_element_type=F32)


def head_cols(idx):
    return slice(idx * HEAD, (idx + 1) * HEAD)


def row_sum(part):
    return jnp.sum(part, axis=-1, keepdims=True)


ANY = pl.BlockSpec(memory_space=pl.ANY)


def place(bits):
    return jnp.where((bits == 0) | (bits == 3), 3 - bits, bits)


def front_own_kernel(*refs):
    dy_ref, *dy_outs = refs[11], *refs[-N_CHUNK:]
    per = pl.num_programs(1) // N_CHUNK
    for c, out_ref in enumerate(dy_outs):
        @pl.when((pl.program_id(0) == 0) & (pl.program_id(1) // per == c))
        def _():
            out_ref[...] = dy_ref[...]

    front_kernel(*refs[:11], *refs[12:-N_CHUNK])


def front_kernel(me_ref, xa_ref, xb_ref, cos_ref, sin_ref, gn_ref, gq_ref, gk_ref, wq_ref, wk_ref, wv_ref, *refs):
    x_ref, h_ref, q_ref, k_ref, v_ref, q1_ref, k1_ref = refs[-7:]
    d_model = x_ref.shape[-1]
    n_heads = d_model // HEAD

    @pl.when(pl.program_id(0) == 0)
    def _():
        x_ref[...] = xa_ref[...]

    @pl.when(pl.program_id(0) == 1)
    def _():
        x_ref[...] = xb_ref[...]

    x_f = x_ref[...].astype(F32)
    inv_x = lax.rsqrt(jnp.mean(x_f * x_f, axis=-1, keepdims=True) + EPS)
    hidden = (x_f * inv_x * gn_ref[...]).astype(BF16)
    blk = d_model // 4
    for b in range(4):
        h_ref[:, pl.ds(pl.multiple_of(place(me_ref[0] ^ b) * blk, blk), blk)] = hidden[:, b * blk:(b + 1) * blk]
    cos_t = cos_ref[...]
    sin_t = sin_ref[...]
    n_col = 512
    for w_ref, g_ref, raw_ref, out_ref in ((wq_ref, gq_ref, q1_ref, q_ref), (wk_ref, gk_ref, k1_ref, k_ref)):
        sq = jnp.zeros((x_ref.shape[0], HEAD), F32)
        for c0 in range(0, d_model, n_col):
            raw = dot_nn(hidden, w_ref[:, c0:c0 + n_col])
            raw_ref[:, c0:c0 + n_col] = raw
            for j in range(n_col // HEAD):
                piece = raw[:, head_cols(j)]
                sq = sq + piece * piece
        inv = lax.rsqrt(row_sum(sq) * (1.0 / d_model) + EPS)
        for j in range(n_heads):
            u = raw_ref[:, head_cols(j)] * inv * g_ref[:, head_cols(j)]
            rot = u * cos_t + pltpu.roll(u, HEAD // 2, 1) * sin_t
            out_ref[:, head_cols(j)] = rot.astype(BF16)
    for c0 in range(0, d_model, n_col):
        v_ref[:, c0:c0 + n_col] = dot_nn(hidden, wv_ref[:, c0:c0 + n_col]).astype(BF16)


def front(me, x_a, x_b, own, bits, seq0, n_seq, cos_t, sin_t, g_norm, g_query, g_key, w_query, w_key, w_value, filled, grad_y=None):
    n_piece, n_all, rows, d_model = cos_t.shape[:3] + x_a.shape[-1:]
    first = lambda i, s: jnp.where(i == 0, s, n_seq - 1)
    second = lambda i, s: jnp.where(i == 0, 0, s)
    x_block = (None, rows, d_model)
    a_map = (lambda i, s, m: (m[0] * n_all + first(i, s), 0, 0)) if own else (lambda i, s, m: (first(i, s), 0, 0))
    spot = lambda i, s, m: (m[0] ^ jnp.where(i == 0, bits[0], bits[1]), seq0 + s, 0, 0)
    table = pl.BlockSpec((None, None, rows, HEAD), spot)
    out = pl.BlockSpec((None, None, rows, d_model), spot)
    vec = pl.BlockSpec((1, d_model), lambda i, s, m: (0, 0))
    mat = pl.BlockSpec((d_model, d_model), lambda i, s, m: (0, 0), pipeline_mode=pl.Buffered(1))
    big = lambda dt: jax.ShapeDtypeStruct((n_piece, n_all, rows, d_model), dt)
    row = lambda g: g.astype(F32).reshape(1, d_model)
    n_tok = 2 * n_seq * rows
    per = n_seq // N_CHUNK

    def own_out(c):
        return pl.BlockSpec((None, None, rows, d_model), lambda i, s, m: (m[0], jnp.clip(first(i, s) - c * per, 0, per - 1), 0, 0))

    dy_in, dy_outs, dy_shapes = [], [], []
    if own:
        dy_in = [pl.BlockSpec(x_block, a_map)]
        dy_outs = [own_out(c) for c in range(N_CHUNK)]
        dy_shapes = [jax.ShapeDtypeStruct((n_piece, per, rows, d_model), BF16)] * N_CHUNK
    return pl.pallas_call(
        front_own_kernel if own else front_kernel,
        grid_spec=pltpu.PrefetchScalarGridSpec(
            num_scalar_prefetch=1,
            grid=(2, n_seq),
            in_specs=[pl.BlockSpec(x_block, a_map), pl.BlockSpec(x_block, lambda i, s, m: (second(i, s), 0, 0)), table, table, vec, vec, vec, mat, mat, mat] + dy_in + [ANY] * len(filled),
            out_specs=[out] * 7 + dy_outs,
        ),
        out_shape=[big(BF16)] * 5 + [big(F32)] * 2 + dy_shapes,
        input_output_aliases={11 + n: n for n in range(len(filled))},
        compiler_params=pltpu.CompilerParams(vmem_limit_bytes=VMEM, dimension_semantics=("arbitrary", "arbitrary")),
        cost_estimate=pl.CostEstimate(flops=6 * n_tok * d_model * d_model, bytes_accessed=n_tok * d_model * 20 + 6 * d_model * d_model, transcendentals=0),
        name="front",
    )(me, x_a, x_b, cos_t, sin_t, row(g_norm), row(g_query), row(g_key), w_query, w_key, w_value, *([grad_y] if own else []), *filled)


def attend_kernel(me_ref, q_ref, k_ref, v_ref, *refs):
    rel_ref, o_ref, lse_ref = refs[-3:]
    n_piece, _, rows, width = q_ref.shape
    keep = lax.broadcasted_iota(jnp.int32, (rows, rows), 0) <= lax.broadcasted_iota(jnp.int32, (rows, rows), 1)
    for hd in range(width // HEAD):
        cols = head_cols(hd)
        v_t = [v_ref[j, 0, :, cols].T for j in range(n_piece)]
        for i in range(n_piece):
            q_i = q_ref[i, 0, :, cols]
            scores = [dot_nt(k_ref[j, 0, :, cols], q_i) for j in range(i + 1)]
            scores[i] = jnp.where(keep, scores[i], NEG_BIG)
            top = scores[0]
            for j in range(1, i + 1):
                top = jnp.maximum(top, scores[j])
            top = jnp.max(top, axis=0, keepdims=True) * SCALE2
            total = None
            out = None
            for j in range(i + 1):
                prob = jnp.exp2(scores[j] * SCALE2 - top)
                part = jnp.sum(prob, axis=0, keepdims=True)
                total = part if total is None else total + part
                term = dot_nn(v_t[j], prob.astype(BF16))
                out = term if out is None else out + term
            out = (out * (1.0 / total)).astype(BF16).T
            o_ref[i, 0, :, cols] = out
            rel_ref[i, 0, :, cols] = out
            lse_ref[0, hd, :, i * rows:(i + 1) * rows] = top + jnp.log2(total)


def attend(me, q_all, k_all, v_all, seq0, n_seq, filled, heads=2):
    n_piece, n_all, rows, d_model = q_all.shape
    n_heads = d_model // HEAD
    per = n_heads // heads // 4
    shape = (n_piece, 1, rows, heads * HEAD)
    blk = pl.BlockSpec(shape, lambda s, h, m: (0, seq0 + s, 0, h))
    rel = pl.BlockSpec(shape, lambda s, h, m: (0, s, 0, place(m[0] ^ (h // per)) * per + h % per))
    seq = n_piece * rows
    big = jax.ShapeDtypeStruct(q_all.shape, BF16)
    return pl.pallas_call(
        attend_kernel,
        grid_spec=pltpu.PrefetchScalarGridSpec(
            num_scalar_prefetch=1,
            grid=(n_seq, n_heads // heads),
            in_specs=[blk] * 3 + [ANY] * len(filled),
            out_specs=[rel, blk, pl.BlockSpec((1, heads, 1, seq), lambda s, h, m: (seq0 + s, h, 0, 0))],
        ),
        out_shape=[jax.ShapeDtypeStruct((n_piece, n_seq, rows, d_model), BF16), big, jax.ShapeDtypeStruct((n_all, n_heads, 1, seq), F32)],
        input_output_aliases={4 + n: n + 1 for n in range(len(filled))},
        compiler_params=pltpu.CompilerParams(vmem_limit_bytes=VMEM, dimension_semantics=("arbitrary", "arbitrary")),
        cost_estimate=pl.CostEstimate(flops=6 * n_seq * seq * seq * d_model, bytes_accessed=10 * n_seq * seq * d_model, transcendentals=0),
        name="attend",
    )(me, q_all, k_all, v_all, *filled)


def attend_back_kernel(q_ref, k_ref, v_ref, do_ref, lse_ref, *refs):
    dq_ref, dk_ref, dv_ref, dk_acc, dv_acc = refs[-5:]
    n_piece, _, rows, width = q_ref.shape
    keep = lax.broadcasted_iota(jnp.int32, (rows, rows), 0) <= lax.broadcasted_iota(jnp.int32, (rows, rows), 1)
    for hd in range(width // HEAD):
        cols = head_cols(hd)
        k_t = [k_ref[j, 0, :, cols].T for j in range(n_piece)]
        for i in range(n_piece):
            q_i = q_ref[i, 0, :, cols]
            do_i = do_ref[i, 0, :, cols]
            lse = lse_ref[0, hd, :, i * rows:(i + 1) * rows]
            probs, d_probs = [], []
            row_dot = None
            for j in range(i + 1):
                prob = jnp.exp2(dot_nt(k_ref[j, 0, :, cols], q_i) * SCALE2 - lse)
                if j == i:
                    prob = jnp.where(keep, prob, 0.0)
                d_prob = dot_nt(v_ref[j, 0, :, cols], do_i)
                part = jnp.sum(prob * d_prob, axis=0, keepdims=True)
                row_dot = part if row_dot is None else row_dot + part
                probs.append(prob)
                d_probs.append(d_prob)
            dq_t = None
            for j in range(i + 1):
                d_s = (probs[j] * (d_probs[j] - row_dot)).astype(BF16)
                dv_term = dot_nn(probs[j].astype(BF16), do_i)
                dk_term = dot_nn(d_s, q_i)
                dq_term = dot_nn(k_t[j], d_s)
                dq_t = dq_term if dq_t is None else dq_t + dq_term
                if i == j:
                    dv_acc[hd, j] = dv_term
                    dk_acc[hd, j] = dk_term
                else:
                    dv_acc[hd, j] += dv_term
                    dk_acc[hd, j] += dk_term
            dq_ref[i, 0, :, cols] = (dq_t * SCALE).astype(BF16).T
        for j in range(n_piece):
            dk_ref[j, 0, :, cols] = (dk_acc[hd, j] * SCALE).astype(BF16)
            dv_ref[j, 0, :, cols] = dv_acc[hd, j].astype(BF16)


def attend_back(q_all, k_all, v_all, d_out, lse, seq0, n_seq, filled, heads=2):
    n_piece, _, rows, d_model = q_all.shape
    n_heads = d_model // HEAD
    shape = (n_piece, 1, rows, heads * HEAD)
    blk = pl.BlockSpec(shape, lambda s, h: (0, seq0 + s, 0, h))
    loc = pl.BlockSpec(shape, lambda s, h: (0, s, 0, h))
    seq = n_piece * rows
    return pl.pallas_call(
        attend_back_kernel,
        grid=(n_seq, n_heads // heads),
        in_specs=[blk] * 3 + [loc, pl.BlockSpec((1, heads, 1, seq), lambda s, h: (seq0 + s, h, 0, 0))] + [ANY] * len(filled),
        out_specs=[loc, loc, blk],
        out_shape=[jax.ShapeDtypeStruct(d_out.shape, BF16)] * 2 + [jax.ShapeDtypeStruct(q_all.shape, BF16)],
        input_output_aliases={5: 2} if filled else {},
        scratch_shapes=[pltpu.VMEM((heads, n_piece, rows, HEAD), F32)] * 2,
        compiler_params=pltpu.CompilerParams(vmem_limit_bytes=VMEM, dimension_semantics=("arbitrary", "arbitrary")),
        cost_estimate=pl.CostEstimate(flops=14 * n_seq * seq * seq * d_model, bytes_accessed=14 * n_seq * seq * d_model, transcendentals=0),
        name="attend_back",
    )(q_all, k_all, v_all, d_out, lse, *filled)


def tail_kernel(dq_ref, dk_ref, dv_ref, q1_ref, k1_ref, x_ref, dy_ref, cos_ref, sin_ref, gn_ref, gq_ref, gk_ref, wq_ref, wk_ref, wv_ref, *refs):
    dqr_ref, dkr_ref, gx_ref, ggn_ref, ggq_ref, ggk_ref, dh_ref, rot_ref = refs[-8:]
    rows, d_model = x_ref.shape
    n_heads = d_model // HEAD
    n_col = 512
    cos_t = cos_ref[...]
    sin_t = sin_ref[...]

    @pl.when((pl.program_id(0) == 0) & (pl.program_id(1) == 0))
    def _():
        for ref in (ggn_ref, ggq_ref, ggk_ref):
            ref[...] = jnp.zeros_like(ref)

    dv_b = dv_ref[...]
    for c0 in range(0, d_model, n_col):
        dh_ref[:, c0:c0 + n_col] = dot_nt(dv_b, wv_ref[c0:c0 + n_col, :])
    for d_ref, raw_ref, g_ref, w_ref, dr_ref, gg_ref in ((dq_ref, q1_ref, gq_ref, wq_ref, dqr_ref, ggq_ref), (dk_ref, k1_ref, gk_ref, wk_ref, dkr_ref, ggk_ref)):
        sq = jnp.zeros((rows, HEAD), F32)
        cross = jnp.zeros((rows, HEAD), F32)
        for j in range(n_heads):
            u = raw_ref[:, head_cols(j)]
            d = d_ref[:, head_cols(j)].astype(F32)
            d = d * cos_t - pltpu.roll(d, HEAD // 2, 1) * sin_t
            rot_ref[:, head_cols(j)] = d
            sq = sq + u * u
            cross = cross + d * g_ref[:, head_cols(j)] * u
        inv = lax.rsqrt(row_sum(sq) * (1.0 / d_model) + EPS)
        coef = row_sum(cross) * (1.0 / d_model) * inv * inv
        for j in range(n_heads):
            u = raw_ref[:, head_cols(j)]
            d = rot_ref[:, head_cols(j)]
            gg_ref[:, head_cols(j)] += jnp.sum(d * (u * inv), axis=0, keepdims=True)
            dr_ref[:, head_cols(j)] = (inv * (d * g_ref[:, head_cols(j)] - u * coef)).astype(BF16)
        d_b = dr_ref[...]
        for c0 in range(0, d_model, n_col):
            dh_ref[:, c0:c0 + n_col] += dot_nt(d_b, w_ref[c0:c0 + n_col, :])
    sq = jnp.zeros((rows, HEAD), F32)
    cross = jnp.zeros((rows, HEAD), F32)
    for j in range(n_heads):
        u = x_ref[:, head_cols(j)].astype(F32)
        sq = sq + u * u
        cross = cross + dh_ref[:, head_cols(j)] * gn_ref[:, head_cols(j)] * u
    inv = lax.rsqrt(row_sum(sq) * (1.0 / d_model) + EPS)
    coef = row_sum(cross) * (1.0 / d_model) * inv * inv
    for j in range(n_heads):
        u = x_ref[:, head_cols(j)].astype(F32)
        d = dh_ref[:, head_cols(j)]
        ggn_ref[:, head_cols(j)] += jnp.sum(d * (u * inv), axis=0, keepdims=True)
        g_x = dy_ref[:, head_cols(j)].astype(F32) + inv * (d * gn_ref[:, head_cols(j)] - u * coef)
        gx_ref[:, head_cols(j)] = g_x.astype(BF16)


def tail(dq, dk, dv, q1, k1, x_all, dy, cos_t, sin_t, g_norm, g_query, g_key, w_query, w_key, w_value, seq0, n_seq, filled):
    n_piece, _, rows, d_model = x_all.shape
    spot = lambda i, s: (i, seq0 + s, 0, 0)
    tok = pl.BlockSpec((None, None, rows, d_model), spot)
    loc = pl.BlockSpec((None, None, rows, d_model), lambda i, s: (i, s, 0, 0))
    table = pl.BlockSpec((None, None, rows, HEAD), spot)
    vec = pl.BlockSpec((1, d_model), lambda i, s: (0, 0))
    mat = pl.BlockSpec((d_model, d_model), lambda i, s: (0, 0), pipeline_mode=pl.Buffered(1))
    big = jax.ShapeDtypeStruct(x_all.shape, BF16)
    small = jax.ShapeDtypeStruct((1, d_model), F32)
    row = lambda g: g.astype(F32).reshape(1, d_model)
    n_tok = n_piece * n_seq * rows
    return pl.pallas_call(
        tail_kernel,
        grid=(n_piece, n_seq),
        in_specs=[loc] * 2 + [tok] * 4 + [loc] + [table] * 2 + [vec] * 3 + [mat] * 3 + [ANY] * len(filled),
        out_specs=[tok] * 3 + [vec] * 3,
        out_shape=[big] * 3 + [small] * 3,
        input_output_aliases={15 + n: n for n in range(len(filled))},
        scratch_shapes=[pltpu.VMEM((rows, d_model), F32)] * 2,
        compiler_params=pltpu.CompilerParams(vmem_limit_bytes=VMEM, dimension_semantics=("arbitrary", "arbitrary")),
        cost_estimate=pl.CostEstimate(flops=6 * n_tok * d_model * d_model, bytes_accessed=n_tok * d_model * 24 + 6 * d_model * d_model, transcendentals=0),
        name="tail",
    )(dq, dk, dv, q1, k1, x_all, dy, cos_t, sin_t, row(g_norm), row(g_query), row(g_key), w_query, w_key, w_value, *filled)


def rope_tables(positions):
    half = HEAD // 2
    inv_freq = ROPE_BASE ** (-jnp.arange(half, dtype=F32) * (2.0 / HEAD))
    angles = positions.astype(F32)[..., None] * inv_freq
    cos_t = jnp.cos(angles)
    sin_t = jnp.sin(angles)
    return jnp.concatenate([cos_t, cos_t], axis=-1), jnp.concatenate([-sin_t, sin_t], axis=-1)


def after(value, *earlier):
    return lax.optimization_barrier((value,) + earlier)[0]


def solution(mesh):
    n_sp = mesh.shape['sp']

    def to_peer(value, bits):
        return lax.ppermute(value, 'sp', [(i, i ^ bits) for i in range(n_sp)])

    def device_step(x_loc, grad_y, positions, g_norm, w_query, w_key, w_value, w_out, g_query, g_key):
        n_batch, rows, d_model = x_loc.shape
        n_seq = n_batch // n_sp
        step = n_seq // N_CHUNK
        me = lax.axis_index('sp')
        me_vec = jnp.reshape(me, (1,)).astype(jnp.int32)
        shape4 = (n_sp, n_seq, rows, d_model)
        flat = lambda arr: arr.reshape(-1, d_model)
        far_bits = (2, 3, 1)

        def piece(arr, bits, seq0, count):
            return lax.dynamic_slice(arr, (me ^ bits, seq0, 0, 0), (1, count, rows, d_model))

        def pieces(arr, seq0, count):
            cut = lax.optimization_barrier((arr,) + tuple(piece(arr, bits, seq0, count) for bits in far_bits))
            return cut[0], cut[1:]

        def send(parts):
            return [to_peer(p, bits) for p, bits in zip(parts, far_bits)]

        def put(buf, got, bits, seq0):
            return lax.dynamic_update_slice(buf, got, (me ^ bits, seq0, 0, 0))

        def grad_rows(rels, rights):
            half = d_model // 2

            def part(cols):
                terms = [dot_tn(flat(r)[:, cols], flat(g)) for r, g in zip(rels, rights)]
                return sum(terms[1:], terms[0])

            out = to_peer(part(slice(0, half)), 1)
            keep = part(slice(half, None))
            far = keep[:half // 2] + out[:half // 2]
            got = to_peer(far, 2)
            return (keep[half // 2:], out[half // 2:], got), far

        pos4 = positions.reshape(n_sp, n_seq, rows)
        pos4, *cut = lax.optimization_barrier([pos4] + [lax.dynamic_slice_in_dim(pos4, me ^ bits, 1, axis=0) for bits in far_bits])
        for bits, got in zip(far_bits, send(cut)):
            pos4 = lax.dynamic_update_slice_in_dim(pos4, got, me ^ bits, axis=0)
        x4 = x_loc.reshape(shape4)
        x_parts = []
        for c in range(N_CHUNK):
            x_parts.append([piece(x4, bits, c * step, step)[0] for bits in (2, 3)])
            x4 = after(x4, *x_parts[-1])
            if c == 0:
                x_near = piece(x4, 1, 0, n_seq)[0]
        x_far = [[to_peer(p, bits) for p, bits in zip(x_parts[c], (2, 3))] for c in range(N_CHUNK)]
        dy4 = after(grad_y.reshape(shape4), x_near, *x_parts[1])
        x_near = to_peer(x_near, 1)
        dy_got = [send([piece(dy4, bits, c * step, step) for bits in far_bits]) for c in range(N_CHUNK)]
        cos_t, sin_t = rope_tables(pos4)
        gains_in = (g_norm, g_query, g_key)
        weights = (w_query, w_key, w_value)
        filled = front(me_vec, x_loc, x_near, True, (0, 1), 0, n_seq, cos_t, sin_t, *gains_in, *weights, (), grad_y)
        filled, dys = filled[:7], list(filled[7:])
        attn = ()
        rels = []
        prev = cos_t
        for c in range(N_CHUNK):
            filled = front(me_vec, x_far[c][0], x_far[c][1], False, (2, 3), c * step, step, after(cos_t, prev), sin_t, *gains_in, *weights, tuple(filled))
            rel, *attn = attend(me_vec, filled[2], filled[3], filled[4], c * step, step, tuple(attn))
            rels.append(rel)
            prev = attn[1]
        x_all, h_rel, q, k, v, q1, k1 = filled
        attn, lse = attn
        y = (flat(x_all).astype(F32) + dot_nn(flat(attn), w_out)).astype(BF16).reshape(shape4)
        y, y_parts = pieces(y, 0, n_seq)
        y_got = send(y_parts)
        prev = y_parts[0]
        dv, tails, gx_got = (), (), []
        gains = 0.0
        for c in range(N_CHUNK):
            dy = dys[c]
            for bits, got in zip(far_bits, dy_got[c]):
                dy = put(dy, after(got, prev), bits, 0)
            dys[c] = dy
            if c == N_CHUNK - 1:
                w_o, prev = grad_rows(rels, dys)
            d_attn = dot_nt(flat(dy), w_out).astype(BF16).reshape(dy.shape)
            dq, dk, *dv = attend_back(q, k, v, d_attn, after(lse, prev), c * step, step, tuple(dv))
            prev = dq
            if c == N_CHUNK - 1:
                w_v, prev = grad_rows([h_rel], dv)
            *tails, ggn, ggq, ggk = tail(dq, dk, dv[0], q1, k1, x_all, dy, after(cos_t, prev), sin_t, *gains_in, *weights, c * step, step, tuple(tails))
            tails[2], gx_parts = pieces(tails[2], c * step, step)
            gx_got.append(send(gx_parts))
            prev = gx_parts[0]
            gains = gains + jnp.concatenate([ggn, ggq, ggk], axis=0)
        dqr, dkr, gx = tails
        w_q, prev = grad_rows([h_rel], [after(dqr, prev)])
        w_k, prev = grad_rows([h_rel], [after(dkr, prev)])
        for bits, got in zip(far_bits, y_got):
            y = put(y, got, bits, 0)
        for c in range(N_CHUNK):
            for bits, got in zip(far_bits, gx_got[c]):
                gx = put(gx, got, bits, c * step)
        gains = gains + to_peer(gains, 1)
        gains = gains + to_peer(gains, 2)
        gains = lax.dynamic_slice_in_dim(gains, me * (d_model // n_sp), d_model // n_sp, axis=1)
        total = lambda terms: terms[0] + terms[1] + terms[2]
        join = lambda arr: arr.reshape(x_loc.shape)
        return (join(y), join(gx), gains[0], total(w_q), total(w_k), total(w_v), total(w_o), gains[1], gains[2])

    seq_spec = P('dp', 'sp', None)
    mat_rep = P(None, None)
    vec_rep = P(None)
    row_spec = P(('dp', 'sp'), None)
    vec_spec = P(('dp', 'sp'))
    return jax.shard_map(device_step, mesh=mesh, in_specs=(seq_spec, seq_spec, P('dp', 'sp'), vec_rep, mat_rep, mat_rep, mat_rep, mat_rep, vec_rep, vec_rep), out_specs=(seq_spec, seq_spec, vec_spec, row_spec, row_spec, row_spec, row_spec, vec_spec, vec_spec), check_vma=False)
```

```python
import math
import jax
import jax.numpy as jnp
from jax import lax
from jax.experimental import pallas as pl
from jax.experimental.pallas import tpu as pltpu
from jax.sharding import PartitionSpec as P


HEAD = 128
EPS = 1e-5
ROPE_BASE = 10000.0
NEG_BIG = -1e30
SCALE = HEAD ** -0.5
SCALE2 = SCALE * math.log2(math.e)
N_CHUNK = 2
VMEM = 66_000_000
F32 = jnp.float32
BF16 = jnp.bfloat16


def dot_nn(a, b):
    return lax.dot_general(a, b, (((1,), (0,)), ((), ())), preferred_element_type=F32)


def dot_nt(a, b):
    return lax.dot_general(a, b, (((1,), (1,)), ((), ())), preferred_element_type=F32)


def dot_tn(a, b):
    return lax.dot_general(a, b, (((0,), (0,)), ((), ())), preferred_element_type=F32)


def head_cols(idx):
    return slice(idx * HEAD, (idx + 1) * HEAD)


def row_sum(part):
    return jnp.sum(part, axis=-1, keepdims=True)


ANY = pl.BlockSpec(memory_space=pl.ANY)


def place(bits):
    return jnp.where((bits == 0) | (bits == 3), 3 - bits, bits)


def front_own_kernel(*refs):
    dy_ref, *dy_outs = refs[11], *refs[-N_CHUNK:]
    per = pl.num_programs(1) // N_CHUNK
    for c, out_ref in enumerate(dy_outs):
        @pl.when((pl.program_id(0) == 0) & (pl.program_id(1) // per == c))
        def _():
            out_ref[...] = dy_ref[...]

    front_kernel(*refs[:11], *refs[12:-N_CHUNK])


def front_kernel(me_ref, xa_ref, xb_ref, cos_ref, sin_ref, gn_ref, gq_ref, gk_ref, wq_ref, wk_ref, wv_ref, *refs):
    x_ref, h_ref, q_ref, k_ref, v_ref, q1_ref, k1_ref = refs[-7:]
    d_model = x_ref.shape[-1]
    n_heads = d_model // HEAD

    @pl.when(pl.program_id(0) == 0)
    def _():
        x_ref[...] = xa_ref[...]

    @pl.when(pl.program_id(0) == 1)
    def _():
        x_ref[...] = xb_ref[...]

    x_f = x_ref[...].astype(F32)
    inv_x = lax.rsqrt(jnp.mean(x_f * x_f, axis=-1, keepdims=True) + EPS)
    hidden = (x_f * inv_x * gn_ref[...]).astype(BF16)
    blk = d_model // 4
    for b in range(4):
        h_ref[:, pl.ds(pl.multiple_of(place(me_ref[0] ^ b) * blk, blk), blk)] = hidden[:, b * blk:(b + 1) * blk]
    cos_t = cos_ref[...]
    sin_t = sin_ref[...]
    n_col = 512
    for w_ref, g_ref, raw_ref, out_ref in ((wq_ref, gq_ref, q1_ref, q_ref), (wk_ref, gk_ref, k1_ref, k_ref)):
        sq = jnp.zeros((x_ref.shape[0], HEAD), F32)
        for c0 in range(0, d_model, n_col):
            raw = dot_nn(hidden, w_ref[:, c0:c0 + n_col])
            raw_ref[:, c0:c0 + n_col] = raw
            for j in range(n_col // HEAD):
                piece = raw[:, head_cols(j)]
                sq = sq + piece * piece
        inv = lax.rsqrt(row_sum(sq) * (1.0 / d_model) + EPS)
        for j in range(n_heads):
            u = raw_ref[:, head_cols(j)] * inv * g_ref[:, head_cols(j)]
            rot = u * cos_t + pltpu.roll(u, HEAD // 2, 1) * sin_t
            out_ref[:, head_cols(j)] = rot.astype(BF16)
    for c0 in range(0, d_model, n_col):
        v_ref[:, c0:c0 + n_col] = dot_nn(hidden, wv_ref[:, c0:c0 + n_col]).astype(BF16)


def front(me, x_a, x_b, own, bits, seq0, n_seq, cos_t, sin_t, g_norm, g_query, g_key, w_query, w_key, w_value, filled, grad_y=None):
    n_piece, n_all, rows, d_model = cos_t.shape[:3] + x_a.shape[-1:]
    first = lambda i, s: jnp.where(i == 0, s, n_seq - 1)
    second = lambda i, s: jnp.where(i == 0, 0, s)
    x_block = (None, rows, d_model)
    a_map = (lambda i, s, m: (m[0] * n_all + first(i, s), 0, 0)) if own else (lambda i, s, m: (first(i, s), 0, 0))
    spot = lambda i, s, m: (m[0] ^ jnp.where(i == 0, bits[0], bits[1]), seq0 + s, 0, 0)
    table = pl.BlockSpec((None, None, rows, HEAD), spot)
    out = pl.BlockSpec((None, None, rows, d_model), spot)
    vec = pl.BlockSpec((1, d_model), lambda i, s, m: (0, 0))
    mat = pl.BlockSpec((d_model, d_model), lambda i, s, m: (0, 0), pipeline_mode=pl.Buffered(1))
    big = lambda dt: jax.ShapeDtypeStruct((n_piece, n_all, rows, d_model), dt)
    row = lambda g: g.astype(F32).reshape(1, d_model)
    n_tok = 2 * n_seq * rows
    per = n_seq // N_CHUNK

    def own_out(c):
        return pl.BlockSpec((None, None, rows, d_model), lambda i, s, m: (m[0], jnp.clip(first(i, s) - c * per, 0, per - 1), 0, 0))

    dy_in, dy_outs, dy_shapes = [], [], []
    if own:
        dy_in = [pl.BlockSpec(x_block, a_map)]
        dy_outs = [own_out(c) for c in range(N_CHUNK)]
        dy_shapes = [jax.ShapeDtypeStruct((n_piece, per, rows, d_model), BF16)] * N_CHUNK
    return pl.pallas_call(
        front_own_kernel if own else front_kernel,
        grid_spec=pltpu.PrefetchScalarGridSpec(
            num_scalar_prefetch=1,
            grid=(2, n_seq),
            in_specs=[pl.BlockSpec(x_block, a_map), pl.BlockSpec(x_block, lambda i, s, m: (second(i, s), 0, 0)), table, table, vec, vec, vec, mat, mat, mat] + dy_in + [ANY] * len(filled),
            out_specs=[out] * 7 + dy_outs,
        ),
        out_shape=[big(BF16)] * 5 + [big(F32)] * 2 + dy_shapes,
        input_output_aliases={11 + n: n for n in range(len(filled))},
        compiler_params=pltpu.CompilerParams(vmem_limit_bytes=VMEM, dimension_semantics=("arbitrary", "arbitrary")),
        cost_estimate=pl.CostEstimate(flops=6 * n_tok * d_model * d_model, bytes_accessed=n_tok * d_model * 20 + 6 * d_model * d_model, transcendentals=0),
        name="front",
    )(me, x_a, x_b, cos_t, sin_t, row(g_norm), row(g_query), row(g_key), w_query, w_key, w_value, *([grad_y] if own else []), *filled)


def attend_kernel(me_ref, q_ref, k_ref, v_ref, *refs):
    rel_ref, o_ref, lse_ref = refs[-3:]
    n_piece, _, rows, width = q_ref.shape
    keep = lax.broadcasted_iota(jnp.int32, (rows, rows), 0) <= lax.broadcasted_iota(jnp.int32, (rows, rows), 1)
    for hd in range(width // HEAD):
        cols = head_cols(hd)
        v_t = [v_ref[j, 0, :, cols].T for j in range(n_piece)]
        for i in range(n_piece):
            q_i = q_ref[i, 0, :, cols]
            scores = [dot_nt(k_ref[j, 0, :, cols], q_i) for j in range(i + 1)]
            scores[i] = jnp.where(keep, scores[i], NEG_BIG)
            top = scores[0]
            for j in range(1, i + 1):
                top = jnp.maximum(top, scores[j])
            top = jnp.max(top, axis=0, keepdims=True) * SCALE2
            total = None
            out = None
            for j in range(i + 1):
                prob = jnp.exp2(scores[j] * SCALE2 - top)
                part = jnp.sum(prob, axis=0, keepdims=True)
                total = part if total is None else total + part
                term = dot_nn(v_t[j], prob.astype(BF16))
                out = term if out is None else out + term
            out = (out * (1.0 / total)).astype(BF16).T
            o_ref[i, 0, :, cols] = out
            rel_ref[i, 0, :, cols] = out
            lse_ref[0, hd, :, i * rows:(i + 1) * rows] = top + jnp.log2(total)


def attend(me, q_all, k_all, v_all, seq0, n_seq, filled, heads=2):
    n_piece, n_all, rows, d_model = q_all.shape
    n_heads = d_model // HEAD
    per = n_heads // heads // 4
    shape = (n_piece, 1, rows, heads * HEAD)
    blk = pl.BlockSpec(shape, lambda s, h, m: (0, seq0 + s, 0, h))
    rel = pl.BlockSpec(shape, lambda s, h, m: (0, s, 0, place(m[0] ^ (h // per)) * per + h % per))
    seq = n_piece * rows
    big = jax.ShapeDtypeStruct(q_all.shape, BF16)
    return pl.pallas_call(
        attend_kernel,
        grid_spec=pltpu.PrefetchScalarGridSpec(
            num_scalar_prefetch=1,
            grid=(n_seq, n_heads // heads),
            in_specs=[blk] * 3 + [ANY] * len(filled),
            out_specs=[rel, blk, pl.BlockSpec((1, heads, 1, seq), lambda s, h, m: (seq0 + s, h, 0, 0))],
        ),
        out_shape=[jax.ShapeDtypeStruct((n_piece, n_seq, rows, d_model), BF16), big, jax.ShapeDtypeStruct((n_all, n_heads, 1, seq), F32)],
        input_output_aliases={4 + n: n + 1 for n in range(len(filled))},
        compiler_params=pltpu.CompilerParams(vmem_limit_bytes=VMEM, dimension_semantics=("arbitrary", "arbitrary")),
        cost_estimate=pl.CostEstimate(flops=6 * n_seq * seq * seq * d_model, bytes_accessed=10 * n_seq * seq * d_model, transcendentals=0),
        name="attend",
    )(me, q_all, k_all, v_all, *filled)


def attend_back_kernel(q_ref, k_ref, v_ref, do_ref, lse_ref, *refs):
    dq_ref, dk_ref, dv_ref, dk_acc, dv_acc = refs[-5:]
    n_piece, _, rows, width = q_ref.shape
    keep = lax.broadcasted_iota(jnp.int32, (rows, rows), 0) <= lax.broadcasted_iota(jnp.int32, (rows, rows), 1)
    for hd in range(width // HEAD):
        cols = head_cols(hd)
        k_t = [k_ref[j, 0, :, cols].T for j in range(n_piece)]
        for i in range(n_piece):
            q_i = q_ref[i, 0, :, cols]
            do_i = do_ref[i, 0, :, cols]
            lse = lse_ref[0, hd, :, i * rows:(i + 1) * rows]
            probs, d_probs = [], []
            row_dot = None
            for j in range(i + 1):
                prob = jnp.exp2(dot_nt(k_ref[j, 0, :, cols], q_i) * SCALE2 - lse)
                if j == i:
                    prob = jnp.where(keep, prob, 0.0)
                d_prob = dot_nt(v_ref[j, 0, :, cols], do_i)
                part = jnp.sum(prob * d_prob, axis=0, keepdims=True)
                row_dot = part if row_dot is None else row_dot + part
                probs.append(prob)
                d_probs.append(d_prob)
            dq_t = None
            for j in range(i + 1):
                d_s = (probs[j] * (d_probs[j] - row_dot)).astype(BF16)
                dv_term = dot_nn(probs[j].astype(BF16), do_i)
                dk_term = dot_nn(d_s, q_i)
                dq_term = dot_nn(k_t[j], d_s)
                dq_t = dq_term if dq_t is None else dq_t + dq_term
                if i == j:
                    dv_acc[hd, j] = dv_term
                    dk_acc[hd, j] = dk_term
                else:
                    dv_acc[hd, j] += dv_term
                    dk_acc[hd, j] += dk_term
            dq_ref[i, 0, :, cols] = (dq_t * SCALE).astype(BF16).T
        for j in range(n_piece):
            dk_ref[j, 0, :, cols] = (dk_acc[hd, j] * SCALE).astype(BF16)
            dv_ref[j, 0, :, cols] = dv_acc[hd, j].astype(BF16)


def attend_back(q_all, k_all, v_all, d_out, lse, seq0, n_seq, filled, heads=2):
    n_piece, _, rows, d_model = q_all.shape
    n_heads = d_model // HEAD
    shape = (n_piece, 1, rows, heads * HEAD)
    blk = pl.BlockSpec(shape, lambda s, h: (0, seq0 + s, 0, h))
    loc = pl.BlockSpec(shape, lambda s, h: (0, s, 0, h))
    seq = n_piece * rows
    return pl.pallas_call(
        attend_back_kernel,
        grid=(n_seq, n_heads // heads),
        in_specs=[blk] * 3 + [loc, pl.BlockSpec((1, heads, 1, seq), lambda s, h: (seq0 + s, h, 0, 0))] + [ANY] * len(filled),
        out_specs=[loc, loc, blk],
        out_shape=[jax.ShapeDtypeStruct(d_out.shape, BF16)] * 2 + [jax.ShapeDtypeStruct(q_all.shape, BF16)],
        input_output_aliases={5: 2} if filled else {},
        scratch_shapes=[pltpu.VMEM((heads, n_piece, rows, HEAD), F32)] * 2,
        compiler_params=pltpu.CompilerParams(vmem_limit_bytes=VMEM, dimension_semantics=("arbitrary", "arbitrary")),
        cost_estimate=pl.CostEstimate(flops=14 * n_seq * seq * seq * d_model, bytes_accessed=14 * n_seq * seq * d_model, transcendentals=0),
        name="attend_back",
    )(q_all, k_all, v_all, d_out, lse, *filled)


def tail_kernel(dq_ref, dk_ref, dv_ref, q1_ref, k1_ref, x_ref, dy_ref, cos_ref, sin_ref, gn_ref, gq_ref, gk_ref, wq_ref, wk_ref, wv_ref, *refs):
    dqr_ref, dkr_ref, gx_ref, ggn_ref, ggq_ref, ggk_ref, dh_ref, rot_ref = refs[-8:]
    rows, d_model = x_ref.shape
    n_heads = d_model // HEAD
    n_col = 512
    cos_t = cos_ref[...]
    sin_t = sin_ref[...]

    @pl.when((pl.program_id(0) == 0) & (pl.program_id(1) == 0))
    def _():
        for ref in (ggn_ref, ggq_ref, ggk_ref):
            ref[...] = jnp.zeros_like(ref)

    dv_b = dv_ref[...]
    for c0 in range(0, d_model, n_col):
        dh_ref[:, c0:c0 + n_col] = dot_nt(dv_b, wv_ref[c0:c0 + n_col, :])
    for d_ref, raw_ref, g_ref, w_ref, dr_ref, gg_ref in ((dq_ref, q1_ref, gq_ref, wq_ref, dqr_ref, ggq_ref), (dk_ref, k1_ref, gk_ref, wk_ref, dkr_ref, ggk_ref)):
        sq = jnp.zeros((rows, HEAD), F32)
        cross = jnp.zeros((rows, HEAD), F32)
        for j in range(n_heads):
            u = raw_ref[:, head_cols(j)]
            d = d_ref[:, head_cols(j)].astype(F32)
            d = d * cos_t - pltpu.roll(d, HEAD // 2, 1) * sin_t
            rot_ref[:, head_cols(j)] = d
            sq = sq + u * u
            cross = cross + d * g_ref[:, head_cols(j)] * u
        inv = lax.rsqrt(row_sum(sq) * (1.0 / d_model) + EPS)
        coef = row_sum(cross) * (1.0 / d_model) * inv * inv
        for j in range(n_heads):
            u = raw_ref[:, head_cols(j)]
            d = rot_ref[:, head_cols(j)]
            gg_ref[:, head_cols(j)] += jnp.sum(d * (u * inv), axis=0, keepdims=True)
            dr_ref[:, head_cols(j)] = (inv * (d * g_ref[:, head_cols(j)] - u * coef)).astype(BF16)
        d_b = dr_ref[...]
        for c0 in range(0, d_model, n_col):
            dh_ref[:, c0:c0 + n_col] += dot_nt(d_b, w_ref[c0:c0 + n_col, :])
    sq = jnp.zeros((rows, HEAD), F32)
    cross = jnp.zeros((rows, HEAD), F32)
    for j in range(n_heads):
        u = x_ref[:, head_cols(j)].astype(F32)
        sq = sq + u * u
        cross = cross + dh_ref[:, head_cols(j)] * gn_ref[:, head_cols(j)] * u
    inv = lax.rsqrt(row_sum(sq) * (1.0 / d_model) + EPS)
    coef = row_sum(cross) * (1.0 / d_model) * inv * inv
    for j in range(n_heads):
        u = x_ref[:, head_cols(j)].astype(F32)
        d = dh_ref[:, head_cols(j)]
        ggn_ref[:, head_cols(j)] += jnp.sum(d * (u * inv), axis=0, keepdims=True)
        g_x = dy_ref[:, head_cols(j)].astype(F32) + inv * (d * gn_ref[:, head_cols(j)] - u * coef)
        gx_ref[:, head_cols(j)] = g_x.astype(BF16)


def tail(dq, dk, dv, q1, k1, x_all, dy, cos_t, sin_t, g_norm, g_query, g_key, w_query, w_key, w_value, seq0, n_seq, filled):
    n_piece, _, rows, d_model = x_all.shape
    spot = lambda i, s: (i, seq0 + s, 0, 0)
    tok = pl.BlockSpec((None, None, rows, d_model), spot)
    loc = pl.BlockSpec((None, None, rows, d_model), lambda i, s: (i, s, 0, 0))
    table = pl.BlockSpec((None, None, rows, HEAD), spot)
    vec = pl.BlockSpec((1, d_model), lambda i, s: (0, 0))
    mat = pl.BlockSpec((d_model, d_model), lambda i, s: (0, 0), pipeline_mode=pl.Buffered(1))
    big = jax.ShapeDtypeStruct(x_all.shape, BF16)
    small = jax.ShapeDtypeStruct((1, d_model), F32)
    row = lambda g: g.astype(F32).reshape(1, d_model)
    n_tok = n_piece * n_seq * rows
    return pl.pallas_call(
        tail_kernel,
        grid=(n_piece, n_seq),
        in_specs=[loc] * 2 + [tok] * 4 + [loc] + [table] * 2 + [vec] * 3 + [mat] * 3 + [ANY] * len(filled),
        out_specs=[tok] * 3 + [vec] * 3,
        out_shape=[big] * 3 + [small] * 3,
        input_output_aliases={15 + n: n for n in range(len(filled))},
        scratch_shapes=[pltpu.VMEM((rows, d_model), F32)] * 2,
        compiler_params=pltpu.CompilerParams(vmem_limit_bytes=VMEM, dimension_semantics=("arbitrary", "arbitrary")),
        cost_estimate=pl.CostEstimate(flops=6 * n_tok * d_model * d_model, bytes_accessed=n_tok * d_model * 24 + 6 * d_model * d_model, transcendentals=0),
        name="tail",
    )(dq, dk, dv, q1, k1, x_all, dy, cos_t, sin_t, row(g_norm), row(g_query), row(g_key), w_query, w_key, w_value, *filled)


def rope_tables(positions):
    half = HEAD // 2
    inv_freq = ROPE_BASE ** (-jnp.arange(half, dtype=F32) * (2.0 / HEAD))
    angles = positions.astype(F32)[..., None] * inv_freq
    cos_t = jnp.cos(angles)
    sin_t = jnp.sin(angles)
    return jnp.concatenate([cos_t, cos_t], axis=-1), jnp.concatenate([-sin_t, sin_t], axis=-1)


def after(value, *earlier):
    return lax.optimization_barrier((value,) + earlier)[0]


def solution(mesh):
    n_sp = mesh.shape['sp']

    def to_peer(value, bits):
        return lax.ppermute(value, 'sp', [(i, i ^ bits) for i in range(n_sp)])

    def device_step(x_loc, grad_y, positions, g_norm, w_query, w_key, w_value, w_out, g_query, g_key):
        n_batch, rows, d_model = x_loc.shape
        n_seq = n_batch // n_sp
        step = n_seq // N_CHUNK
        me = lax.axis_index('sp')
        me_vec = jnp.reshape(me, (1,)).astype(jnp.int32)
        shape4 = (n_sp, n_seq, rows, d_model)
        flat = lambda arr: arr.reshape(-1, d_model)
        far_bits = (2, 3, 1)

        def piece(arr, bits, seq0, count):
            return lax.dynamic_slice(arr, (me ^ bits, seq0, 0, 0), (1, count, rows, d_model))

        def pieces(arr, seq0, count):
            cut = lax.optimization_barrier((arr,) + tuple(piece(arr, bits, seq0, count) for bits in far_bits))
            return cut[0], cut[1:]

        def send(parts):
            return [to_peer(p, bits) for p, bits in zip(parts, far_bits)]

        def put(buf, got, bits, seq0):
            return lax.dynamic_update_slice(buf, got, (me ^ bits, seq0, 0, 0))

        def grad_rows(rels, rights):
            half = d_model // 2

            def part(cols):
                terms = [dot_tn(flat(r)[:, cols], flat(g)) for r, g in zip(rels, rights)]
                return sum(terms[1:], terms[0])

            out = part(slice(0, half))
            out = to_peer(out, 1)
            keep = part(slice(half, None))
            far = keep[:half // 2] + out[:half // 2]
            got = to_peer(far, 2)
            return (keep[half // 2:], out[half // 2:], got), far

        pos4 = positions.reshape(n_sp, n_seq, rows)
        pos4, *cut = lax.optimization_barrier([pos4] + [lax.dynamic_slice_in_dim(pos4, me ^ bits, 1, axis=0) for bits in far_bits])
        for bits, got in zip(far_bits, send(cut)):
            pos4 = lax.dynamic_update_slice_in_dim(pos4, got, me ^ bits, axis=0)
        x4 = x_loc.reshape(shape4)
        x_parts = []
        x_near = piece(x4, 1, 0, n_seq)[0]
        x4 = after(x4, x_near)
        for c in range(N_CHUNK):
            x_parts.append([piece(x4, bits, c * step, step)[0] for bits in (2, 3)])
            x4 = after(x4, *x_parts[-1])
        x_far = [[to_peer(p, bits) for p, bits in zip(x_parts[c], (2, 3))] for c in range(N_CHUNK)]
        dy4 = after(grad_y.reshape(shape4), *x_parts[1])
        x_near = to_peer(x_near, 1)
        dy_got = [send([piece(dy4, bits, c * step, step) for bits in far_bits]) for c in range(N_CHUNK)]
        cos_t, sin_t = rope_tables(pos4)
        gains_in = (g_norm, g_query, g_key)
        weights = (w_query, w_key, w_value)
        filled = front(me_vec, x_loc, x_near, True, (0, 1), 0, n_seq, cos_t, sin_t, *gains_in, *weights, (), grad_y)
        filled, dys = filled[:7], list(filled[7:])
        attn = ()
        rels = []
        prev = cos_t
        for c in range(N_CHUNK):
            filled = front(me_vec, x_far[c][0], x_far[c][1], False, (2, 3), c * step, step, after(cos_t, prev), sin_t, *gains_in, *weights, tuple(filled))
            rel, *attn = attend(me_vec, filled[2], filled[3], filled[4], c * step, step, tuple(attn))
            rels.append(rel)
            prev = attn[1]
        x_all, h_rel, q, k, v, q1, k1 = filled
        attn, lse = attn
        y = (flat(x_all).astype(F32) + dot_nn(flat(attn), w_out)).astype(BF16).reshape(shape4)
        y, y_parts = pieces(y, 0, n_seq)
        y_got = send(y_parts)
        prev = y_parts[0]
        dv, tails, gx_got, dqk = (), (), [], []
        for c in range(N_CHUNK):
            dy = dys[c]
            for bits, got in zip(far_bits, dy_got[c]):
                dy = put(dy, after(got, prev), bits, 0)
            dys[c] = dy
            if c == N_CHUNK - 1:
                w_o, prev = grad_rows(rels, dys)
            d_attn = dot_nt(flat(dy), w_out).astype(BF16).reshape(dy.shape)
            dq, dk, *dv = attend_back(q, k, v, d_attn, after(lse, prev), c * step, step, tuple(dv))
            dqk.append((dq, dk))
            prev = dq
        w_v, prev = grad_rows([h_rel], dv)
        gains = 0.0
        for c in range(N_CHUNK):
            *tails, ggn, ggq, ggk = tail(*dqk[c], dv[0], q1, k1, x_all, dys[c], after(cos_t, prev), sin_t, *gains_in, *weights, c * step, step, tuple(tails))
            gains = gains + jnp.concatenate([ggn, ggq, ggk], axis=0)
            tails[2], gx_parts = pieces(tails[2], c * step, step)
            if c == N_CHUNK - 1:
                gains = gains + to_peer(gains, 2)
            gx_got.append(send(gx_parts))
            prev = gx_parts[0]
        dqr, dkr, gx = tails
        w_q, prev = grad_rows([h_rel], [after(dqr, prev)])
        w_k, prev = grad_rows([h_rel], [after(dkr, prev)])
        for bits, got in zip(far_bits, y_got):
            y = put(y, after(got, prev), bits, 0)
        for c in range(N_CHUNK):
            for bits, got in zip(far_bits, gx_got[c]):
                gx = put(gx, got, bits, c * step)
        gains = gains + to_peer(gains, 1)
        gains = lax.dynamic_slice_in_dim(gains, me * (d_model // n_sp), d_model // n_sp, axis=1)
        total = lambda terms: terms[0] + terms[1] + terms[2]
        join = lambda arr: arr.reshape(x_loc.shape)
        return (join(y), join(gx), gains[0], total(w_q), total(w_k), total(w_v), total(w_o), gains[1], gains[2])

    seq_spec = P('dp', 'sp', None)
    mat_rep = P(None, None)
    vec_rep = P(None)
    row_spec = P(('dp', 'sp'), None)
    vec_spec = P(('dp', 'sp'))
    return jax.shard_map(device_step, mesh=mesh, in_specs=(seq_spec, seq_spec, P('dp', 'sp'), vec_rep, mat_rep, mat_rep, mat_rep, mat_rep, vec_rep, vec_rep), out_specs=(seq_spec, seq_spec, vec_spec, row_spec, row_spec, row_spec, row_spec, vec_spec, vec_spec), check_vma=False)
```

```python
import math
import jax
import jax.numpy as jnp
from jax import lax
from jax.experimental import pallas as pl
from jax.experimental.pallas import tpu as pltpu
from jax.sharding import PartitionSpec as P


HEAD = 128
EPS = 1e-5
ROPE_BASE = 10000.0
NEG_BIG = -1e30
SCALE = HEAD ** -0.5
SCALE2 = SCALE * math.log2(math.e)
N_CHUNK = 2
VMEM = 66_000_000
F32 = jnp.float32
BF16 = jnp.bfloat16


def dot_nn(a, b):
    return lax.dot_general(a, b, (((1,), (0,)), ((), ())), preferred_element_type=F32)


def dot_nt(a, b):
    return lax.dot_general(a, b, (((1,), (1,)), ((), ())), preferred_element_type=F32)


def dot_tn(a, b):
    return lax.dot_general(a, b, (((0,), (0,)), ((), ())), preferred_element_type=F32)


def head_cols(idx):
    return slice(idx * HEAD, (idx + 1) * HEAD)


def row_sum(part):
    return jnp.sum(part, axis=-1, keepdims=True)


ANY = pl.BlockSpec(memory_space=pl.ANY)


def place(bits):
    return 3 - bits


def front_own_kernel(*refs):
    dy_ref, *dy_outs = refs[11], *refs[-N_CHUNK:]
    per = pl.num_programs(1) // N_CHUNK
    for c, out_ref in enumerate(dy_outs):
        @pl.when((pl.program_id(0) == 0) & (pl.program_id(1) // per == c))
        def _():
            out_ref[...] = dy_ref[...]

    front_kernel(*refs[:11], *refs[12:-N_CHUNK])


def front_kernel(me_ref, xa_ref, xb_ref, cos_ref, sin_ref, gn_ref, gq_ref, gk_ref, wq_ref, wk_ref, wv_ref, *refs):
    x_ref, h_ref, q_ref, k_ref, v_ref, q1_ref, k1_ref = refs[-7:]
    d_model = x_ref.shape[-1]
    n_heads = d_model // HEAD

    @pl.when(pl.program_id(0) == 0)
    def _():
        x_ref[...] = xa_ref[...]

    @pl.when(pl.program_id(0) == 1)
    def _():
        x_ref[...] = xb_ref[...]

    x_f = x_ref[...].astype(F32)
    inv_x = lax.rsqrt(jnp.mean(x_f * x_f, axis=-1, keepdims=True) + EPS)
    hidden = (x_f * inv_x * gn_ref[...]).astype(BF16)
    blk = d_model // 4
    for b in range(4):
        h_ref[:, pl.ds(pl.multiple_of(place(me_ref[0] ^ b) * blk, blk), blk)] = hidden[:, b * blk:(b + 1) * blk]
    cos_t = cos_ref[...]
    sin_t = sin_ref[...]
    n_col = 512
    for w_ref, g_ref, raw_ref, out_ref in ((wq_ref, gq_ref, q1_ref, q_ref), (wk_ref, gk_ref, k1_ref, k_ref)):
        sq = jnp.zeros((x_ref.shape[0], HEAD), F32)
        for c0 in range(0, d_model, n_col):
            raw = dot_nn(hidden, w_ref[:, c0:c0 + n_col])
            raw_ref[:, c0:c0 + n_col] = raw
            for j in range(n_col // HEAD):
                piece = raw[:, head_cols(j)]
                sq = sq + piece * piece
        inv = lax.rsqrt(row_sum(sq) * (1.0 / d_model) + EPS)
        for j in range(n_heads):
            u = raw_ref[:, head_cols(j)] * inv * g_ref[:, head_cols(j)]
            rot = u * cos_t + pltpu.roll(u, HEAD // 2, 1) * sin_t
            out_ref[:, head_cols(j)] = rot.astype(BF16)
    for c0 in range(0, d_model, n_col):
        v_ref[:, c0:c0 + n_col] = dot_nn(hidden, wv_ref[:, c0:c0 + n_col]).astype(BF16)


def front(me, x_a, x_b, own, bits, seq0, n_seq, cos_t, sin_t, g_norm, g_query, g_key, w_query, w_key, w_value, filled, grad_y=None):
    n_piece, n_all, rows, d_model = cos_t.shape[:3] + x_a.shape[-1:]
    first = lambda i, s: jnp.where(i == 0, s, n_seq - 1)
    second = lambda i, s: jnp.where(i == 0, 0, s)
    x_block = (None, rows, d_model)
    a_map = (lambda i, s, m: (m[0] * n_all + first(i, s), 0, 0)) if own else (lambda i, s, m: (first(i, s), 0, 0))
    spot = lambda i, s, m: (m[0] ^ jnp.where(i == 0, bits[0], bits[1]), seq0 + s, 0, 0)
    table = pl.BlockSpec((None, None, rows, HEAD), spot)
    out = pl.BlockSpec((None, None, rows, d_model), spot)
    vec = pl.BlockSpec((1, d_model), lambda i, s, m: (0, 0))
    mat = pl.BlockSpec((d_model, d_model), lambda i, s, m: (0, 0), pipeline_mode=pl.Buffered(1))
    big = lambda dt: jax.ShapeDtypeStruct((n_piece, n_all, rows, d_model), dt)
    row = lambda g: g.astype(F32).reshape(1, d_model)
    n_tok = 2 * n_seq * rows
    per = n_seq // N_CHUNK

    def own_out(c):
        return pl.BlockSpec((None, None, rows, d_model), lambda i, s, m: (m[0], jnp.clip(first(i, s) - c * per, 0, per - 1), 0, 0))

    dy_in, dy_outs, dy_shapes = [], [], []
    if own:
        dy_in = [pl.BlockSpec(x_block, a_map)]
        dy_outs = [own_out(c) for c in range(N_CHUNK)]
        dy_shapes = [jax.ShapeDtypeStruct((n_piece, per, rows, d_model), BF16)] * N_CHUNK
    return pl.pallas_call(
        front_own_kernel if own else front_kernel,
        grid_spec=pltpu.PrefetchScalarGridSpec(
            num_scalar_prefetch=1,
            grid=(2, n_seq),
            in_specs=[pl.BlockSpec(x_block, a_map), pl.BlockSpec(x_block, lambda i, s, m: (second(i, s), 0, 0)), table, table, vec, vec, vec, mat, mat, mat] + dy_in + [ANY] * len(filled),
            out_specs=[out] * 7 + dy_outs,
        ),
        out_shape=[big(BF16)] * 5 + [big(F32)] * 2 + dy_shapes,
        input_output_aliases={11 + n: n for n in range(len(filled))},
        compiler_params=pltpu.CompilerParams(vmem_limit_bytes=VMEM, dimension_semantics=("arbitrary", "arbitrary")),
        cost_estimate=pl.CostEstimate(flops=6 * n_tok * d_model * d_model, bytes_accessed=n_tok * d_model * 20 + 6 * d_model * d_model, transcendentals=0),
        name="front",
    )(me, x_a, x_b, cos_t, sin_t, row(g_norm), row(g_query), row(g_key), w_query, w_key, w_value, *([grad_y] if own else []), *filled)


def attend_kernel(me_ref, q_ref, k_ref, v_ref, *refs):
    rel_ref, o_ref, lse_ref = refs[-3:]
    n_piece, _, rows, width = q_ref.shape
    keep = lax.broadcasted_iota(jnp.int32, (rows, rows), 0) <= lax.broadcasted_iota(jnp.int32, (rows, rows), 1)
    for hd in range(width // HEAD):
        cols = head_cols(hd)
        v_t = [v_ref[j, 0, :, cols].T for j in range(n_piece)]
        for i in range(n_piece):
            q_i = q_ref[i, 0, :, cols]
            scores = [dot_nt(k_ref[j, 0, :, cols], q_i) for j in range(i + 1)]
            scores[i] = jnp.where(keep, scores[i], NEG_BIG)
            top = scores[0]
            for j in range(1, i + 1):
                top = jnp.maximum(top, scores[j])
            top = jnp.max(top, axis=0, keepdims=True) * SCALE2
            total = None
            out = None
            for j in range(i + 1):
                prob = jnp.exp2(scores[j] * SCALE2 - top)
                part = jnp.sum(prob, axis=0, keepdims=True)
                total = part if total is None else total + part
                term = dot_nn(v_t[j], prob.astype(BF16))
                out = term if out is None else out + term
            out = (out * (1.0 / total)).astype(BF16).T
            o_ref[i, 0, :, cols] = out
            rel_ref[i, 0, :, cols] = out
            lse_ref[0, hd, :, i * rows:(i + 1) * rows] = top + jnp.log2(total)


def attend(me, q_all, k_all, v_all, seq0, n_seq, filled, heads=2):
    n_piece, n_all, rows, d_model = q_all.shape
    n_heads = d_model // HEAD
    per = n_heads // heads // 4
    shape = (n_piece, 1, rows, heads * HEAD)
    blk = pl.BlockSpec(shape, lambda s, h, m: (0, seq0 + s, 0, h))
    rel = pl.BlockSpec(shape, lambda s, h, m: (0, s, 0, place(m[0] ^ (h // per)) * per + h % per))
    seq = n_piece * rows
    big = jax.ShapeDtypeStruct(q_all.shape, BF16)
    return pl.pallas_call(
        attend_kernel,
        grid_spec=pltpu.PrefetchScalarGridSpec(
            num_scalar_prefetch=1,
            grid=(n_seq, n_heads // heads),
            in_specs=[blk] * 3 + [ANY] * len(filled),
            out_specs=[rel, blk, pl.BlockSpec((1, heads, 1, seq), lambda s, h, m: (seq0 + s, h, 0, 0))],
        ),
        out_shape=[jax.ShapeDtypeStruct((n_piece, n_seq, rows, d_model), BF16), big, jax.ShapeDtypeStruct((n_all, n_heads, 1, seq), F32)],
        input_output_aliases={4 + n: n + 1 for n in range(len(filled))},
        compiler_params=pltpu.CompilerParams(vmem_limit_bytes=VMEM, dimension_semantics=("arbitrary", "arbitrary")),
        cost_estimate=pl.CostEstimate(flops=6 * n_seq * seq * seq * d_model, bytes_accessed=10 * n_seq * seq * d_model, transcendentals=0),
        name="attend",
    )(me, q_all, k_all, v_all, *filled)


def attend_back_kernel(q_ref, k_ref, v_ref, do_ref, lse_ref, *refs):
    dq_ref, dk_ref, dv_ref, dk_acc, dv_acc = refs[-5:]
    n_piece, _, rows, width = q_ref.shape
    keep = lax.broadcasted_iota(jnp.int32, (rows, rows), 0) <= lax.broadcasted_iota(jnp.int32, (rows, rows), 1)
    for hd in range(width // HEAD):
        cols = head_cols(hd)
        k_t = [k_ref[j, 0, :, cols].T for j in range(n_piece)]
        for i in range(n_piece):
            q_i = q_ref[i, 0, :, cols]
            do_i = do_ref[i, 0, :, cols]
            lse = lse_ref[0, hd, :, i * rows:(i + 1) * rows]
            probs, d_probs = [], []
            row_dot = None
            for j in range(i + 1):
                prob = jnp.exp2(dot_nt(k_ref[j, 0, :, cols], q_i) * SCALE2 - lse)
                if j == i:
                    prob = jnp.where(keep, prob, 0.0)
                d_prob = dot_nt(v_ref[j, 0, :, cols], do_i)
                part = jnp.sum(prob * d_prob, axis=0, keepdims=True)
                row_dot = part if row_dot is None else row_dot + part
                probs.append(prob)
                d_probs.append(d_prob)
            dq_t = None
            for j in range(i + 1):
                d_s = (probs[j] * (d_probs[j] - row_dot)).astype(BF16)
                dv_term = dot_nn(probs[j].astype(BF16), do_i)
                dk_term = dot_nn(d_s, q_i)
                dq_term = dot_nn(k_t[j], d_s)
                dq_t = dq_term if dq_t is None else dq_t + dq_term
                if i == j:
                    dv_acc[hd, j] = dv_term
                    dk_acc[hd, j] = dk_term
                else:
                    dv_acc[hd, j] += dv_term
                    dk_acc[hd, j] += dk_term
            dq_ref[i, 0, :, cols] = (dq_t * SCALE).astype(BF16).T
        for j in range(n_piece):
            dk_ref[j, 0, :, cols] = (dk_acc[hd, j] * SCALE).astype(BF16)
            dv_ref[j, 0, :, cols] = dv_acc[hd, j].astype(BF16)


def attend_back(q_all, k_all, v_all, d_out, lse, seq0, n_seq, filled, heads=2):
    n_piece, _, rows, d_model = q_all.shape
    n_heads = d_model // HEAD
    shape = (n_piece, 1, rows, heads * HEAD)
    blk = pl.BlockSpec(shape, lambda s, h: (0, seq0 + s, 0, h))
    loc = pl.BlockSpec(shape, lambda s, h: (0, s, 0, h))
    seq = n_piece * rows
    return pl.pallas_call(
        attend_back_kernel,
        grid=(n_seq, n_heads // heads),
        in_specs=[blk] * 3 + [loc, pl.BlockSpec((1, heads, 1, seq), lambda s, h: (seq0 + s, h, 0, 0))] + [ANY] * len(filled),
        out_specs=[loc, loc, blk],
        out_shape=[jax.ShapeDtypeStruct(d_out.shape, BF16)] * 2 + [jax.ShapeDtypeStruct(q_all.shape, BF16)],
        input_output_aliases={5: 2} if filled else {},
        scratch_shapes=[pltpu.VMEM((heads, n_piece, rows, HEAD), F32)] * 2,
        compiler_params=pltpu.CompilerParams(vmem_limit_bytes=VMEM, dimension_semantics=("arbitrary", "arbitrary")),
        cost_estimate=pl.CostEstimate(flops=14 * n_seq * seq * seq * d_model, bytes_accessed=14 * n_seq * seq * d_model, transcendentals=0),
        name="attend_back",
    )(q_all, k_all, v_all, d_out, lse, *filled)


def tail_kernel(dq_ref, dk_ref, dv_ref, q1_ref, k1_ref, x_ref, dy_ref, cos_ref, sin_ref, gn_ref, gq_ref, gk_ref, wq_ref, wk_ref, wv_ref, *refs):
    dqr_ref, dkr_ref, gx_ref, ggn_ref, ggq_ref, ggk_ref, dh_ref, rot_ref = refs[-8:]
    rows, d_model = x_ref.shape
    n_heads = d_model // HEAD
    n_col = 512
    cos_t = cos_ref[...]
    sin_t = sin_ref[...]

    @pl.when((pl.program_id(0) == 0) & (pl.program_id(1) == 0))
    def _():
        for ref in (ggn_ref, ggq_ref, ggk_ref):
            ref[...] = jnp.zeros_like(ref)

    dv_b = dv_ref[...]
    for c0 in range(0, d_model, n_col):
        dh_ref[:, c0:c0 + n_col] = dot_nt(dv_b, wv_ref[c0:c0 + n_col, :])
    for d_ref, raw_ref, g_ref, w_ref, dr_ref, gg_ref in ((dq_ref, q1_ref, gq_ref, wq_ref, dqr_ref, ggq_ref), (dk_ref, k1_ref, gk_ref, wk_ref, dkr_ref, ggk_ref)):
        sq = jnp.zeros((rows, HEAD), F32)
        cross = jnp.zeros((rows, HEAD), F32)
        for j in range(n_heads):
            u = raw_ref[:, head_cols(j)]
            d = d_ref[:, head_cols(j)].astype(F32)
            d = d * cos_t - pltpu.roll(d, HEAD // 2, 1) * sin_t
            rot_ref[:, head_cols(j)] = d
            sq = sq + u * u
            cross = cross + d * g_ref[:, head_cols(j)] * u
        inv = lax.rsqrt(row_sum(sq) * (1.0 / d_model) + EPS)
        coef = row_sum(cross) * (1.0 / d_model) * inv * inv
        for j in range(n_heads):
            u = raw_ref[:, head_cols(j)]
            d = rot_ref[:, head_cols(j)]
            gg_ref[:, head_cols(j)] += jnp.sum(d * (u * inv), axis=0, keepdims=True)
            dr_ref[:, head_cols(j)] = (inv * (d * g_ref[:, head_cols(j)] - u * coef)).astype(BF16)
        d_b = dr_ref[...]
        for c0 in range(0, d_model, n_col):
            dh_ref[:, c0:c0 + n_col] += dot_nt(d_b, w_ref[c0:c0 + n_col, :])
    sq = jnp.zeros((rows, HEAD), F32)
    cross = jnp.zeros((rows, HEAD), F32)
    for j in range(n_heads):
        u = x_ref[:, head_cols(j)].astype(F32)
        sq = sq + u * u
        cross = cross + dh_ref[:, head_cols(j)] * gn_ref[:, head_cols(j)] * u
    inv = lax.rsqrt(row_sum(sq) * (1.0 / d_model) + EPS)
    coef = row_sum(cross) * (1.0 / d_model) * inv * inv
    for j in range(n_heads):
        u = x_ref[:, head_cols(j)].astype(F32)
        d = dh_ref[:, head_cols(j)]
        ggn_ref[:, head_cols(j)] += jnp.sum(d * (u * inv), axis=0, keepdims=True)
        g_x = dy_ref[:, head_cols(j)].astype(F32) + inv * (d * gn_ref[:, head_cols(j)] - u * coef)
        gx_ref[:, head_cols(j)] = g_x.astype(BF16)


def tail(dq, dk, dv, q1, k1, x_all, dy, cos_t, sin_t, g_norm, g_query, g_key, w_query, w_key, w_value, seq0, n_seq, filled):
    n_piece, _, rows, d_model = x_all.shape
    spot = lambda i, s: (i, seq0 + s, 0, 0)
    tok = pl.BlockSpec((None, None, rows, d_model), spot)
    loc = pl.BlockSpec((None, None, rows, d_model), lambda i, s: (i, s, 0, 0))
    table = pl.BlockSpec((None, None, rows, HEAD), spot)
    vec = pl.BlockSpec((1, d_model), lambda i, s: (0, 0))
    mat = pl.BlockSpec((d_model, d_model), lambda i, s: (0, 0), pipeline_mode=pl.Buffered(1))
    big = jax.ShapeDtypeStruct(x_all.shape, BF16)
    small = jax.ShapeDtypeStruct((1, d_model), F32)
    row = lambda g: g.astype(F32).reshape(1, d_model)
    n_tok = n_piece * n_seq * rows
    return pl.pallas_call(
        tail_kernel,
        grid=(n_piece, n_seq),
        in_specs=[loc] * 2 + [tok] * 4 + [loc] + [table] * 2 + [vec] * 3 + [mat] * 3 + [ANY] * len(filled),
        out_specs=[tok] * 3 + [vec] * 3,
        out_shape=[big] * 3 + [small] * 3,
        input_output_aliases={15 + n: n for n in range(len(filled))},
        scratch_shapes=[pltpu.VMEM((rows, d_model), F32)] * 2,
        compiler_params=pltpu.CompilerParams(vmem_limit_bytes=VMEM, dimension_semantics=("arbitrary", "arbitrary")),
        cost_estimate=pl.CostEstimate(flops=6 * n_tok * d_model * d_model, bytes_accessed=n_tok * d_model * 24 + 6 * d_model * d_model, transcendentals=0),
        name="tail",
    )(dq, dk, dv, q1, k1, x_all, dy, cos_t, sin_t, row(g_norm), row(g_query), row(g_key), w_query, w_key, w_value, *filled)


def rope_tables(positions):
    half = HEAD // 2
    inv_freq = ROPE_BASE ** (-jnp.arange(half, dtype=F32) * (2.0 / HEAD))
    angles = positions.astype(F32)[..., None] * inv_freq
    cos_t = jnp.cos(angles)
    sin_t = jnp.sin(angles)
    return jnp.concatenate([cos_t, cos_t], axis=-1), jnp.concatenate([-sin_t, sin_t], axis=-1)


def after(value, *earlier):
    return lax.optimization_barrier((value,) + earlier)[0]


def solution(mesh):
    n_sp = mesh.shape['sp']

    def to_peer(value, bits):
        return lax.ppermute(value, 'sp', [(i, i ^ bits) for i in range(n_sp)])

    def device_step(x_loc, grad_y, positions, g_norm, w_query, w_key, w_value, w_out, g_query, g_key):
        n_batch, rows, d_model = x_loc.shape
        n_seq = n_batch // n_sp
        step = n_seq // N_CHUNK
        me = lax.axis_index('sp')
        me_vec = jnp.reshape(me, (1,)).astype(jnp.int32)
        shape4 = (n_sp, n_seq, rows, d_model)
        flat = lambda arr: arr.reshape(-1, d_model)
        far_bits = (2, 3, 1)

        def piece(arr, bits, seq0, count):
            return lax.dynamic_slice(arr, (me ^ bits, seq0, 0, 0), (1, count, rows, d_model))

        def pieces(arr, seq0, count):
            cut = lax.optimization_barrier((arr,) + tuple(piece(arr, bits, seq0, count) for bits in far_bits))
            return cut[0], cut[1:]

        def send(parts):
            return [to_peer(p, bits) for p, bits in zip(parts, far_bits)]

        def put(buf, got, bits, seq0):
            return lax.dynamic_update_slice(buf, got, (me ^ bits, seq0, 0, 0))

        def grad_rows(rels, rights):
            blk = d_model // n_sp

            def part(n, grads):
                terms = [dot_tn(flat(r)[:, n * blk:(n + 1) * blk], flat(g)) for r, g in zip(rels, grads)]
                return sum(terms[1:], terms[0])

            given = to_peer(part(0, rights), 1)
            far = lax.optimization_barrier(part(1, rights)) + given
            got = to_peer(far, 2)

            def rest(prev):
                late = [after(g, prev) for g in rights]
                given = to_peer(part(2, late), 1)
                mine = lax.optimization_barrier(part(3, late))
                return mine, given, got

            return rest, far

        pos4 = positions.reshape(n_sp, n_seq, rows)
        pos4, *cut = lax.optimization_barrier([pos4] + [lax.dynamic_slice_in_dim(pos4, me ^ bits, 1, axis=0) for bits in far_bits])
        for bits, got in zip(far_bits, send(cut)):
            pos4 = lax.dynamic_update_slice_in_dim(pos4, got, me ^ bits, axis=0)
        x4 = x_loc.reshape(shape4)
        x_parts = []
        x_near = piece(x4, 1, 0, n_seq)[0]
        x4 = after(x4, x_near)
        for c in range(N_CHUNK):
            x_parts.append([piece(x4, bits, c * step, step)[0] for bits in (2, 3)])
            x4 = after(x4, *x_parts[-1])
        x_far = [[to_peer(p, bits) for p, bits in zip(x_parts[c], (2, 3))] for c in range(N_CHUNK)]
        dy4 = after(grad_y.reshape(shape4), *x_parts[1])
        x_near = to_peer(x_near, 1)
        dy_got = [send([piece(dy4, bits, c * step, step) for bits in far_bits]) for c in range(N_CHUNK)]
        cos_t, sin_t = rope_tables(pos4)
        gains_in = (g_norm, g_query, g_key)
        weights = (w_query, w_key, w_value)
        filled = front(me_vec, x_loc, x_near, True, (0, 1), 0, n_seq, cos_t, sin_t, *gains_in, *weights, (), grad_y)
        filled, dys = filled[:7], list(filled[7:])
        attn = ()
        rels = []
        prev = cos_t
        for c in range(N_CHUNK):
            filled = front(me_vec, x_far[c][0], x_far[c][1], False, (2, 3), c * step, step, after(cos_t, prev), sin_t, *gains_in, *weights, tuple(filled))
            rel, *attn = attend(me_vec, filled[2], filled[3], filled[4], c * step, step, tuple(attn))
            rels.append(rel)
            prev = attn[1]
        x_all, h_rel, q, k, v, q1, k1 = filled
        attn, lse = attn
        y = (flat(x_all).astype(F32) + dot_nn(flat(attn), w_out)).astype(BF16).reshape(shape4)
        y, y_parts = pieces(y, 0, n_seq)
        y_got = send(y_parts)
        prev = y_parts[0]
        dv, tails, gx_got, dqk = (), (), [], []
        for c in range(N_CHUNK):
            dy = dys[c]
            for bits, got in zip(far_bits, dy_got[c]):
                dy = put(dy, after(got, prev), bits, 0)
            dys[c] = dy
            if c == N_CHUNK - 1:
                w_o, prev = grad_rows(rels, dys)
            d_attn = dot_nt(flat(dy), w_out).astype(BF16).reshape(dy.shape)
            dq, dk, *dv = attend_back(q, k, v, d_attn, after(lse, prev), c * step, step, tuple(dv))
            dqk.append((dq, dk))
            prev = dq
        w_v, prev = grad_rows([h_rel], dv)
        gains = 0.0
        for c in range(N_CHUNK):
            *tails, ggn, ggq, ggk = tail(*dqk[c], dv[0], q1, k1, x_all, dys[c], after(cos_t, prev), sin_t, *gains_in, *weights, c * step, step, tuple(tails))
            gains = gains + jnp.concatenate([ggn, ggq, ggk], axis=0)
            tails[2], gx_parts = pieces(tails[2], c * step, step)
            if c == N_CHUNK - 1:
                gains = gains + to_peer(gains, 2)
            gx_got.append(send(gx_parts))
            prev = gx_parts[0]
        dqr, dkr, gx = tails
        w_q, prev = grad_rows([h_rel], [after(dqr, prev)])
        w_k, prev = grad_rows([h_rel], [after(dkr, prev)])
        sums = []
        for rest in (w_q, w_k, w_v, w_o):
            sums.append(rest(prev))
            prev = sums[-1][0]
        for bits, got in zip(far_bits, y_got):
            y = put(y, after(got, prev), bits, 0)
        for c in range(N_CHUNK):
            for bits, got in zip(far_bits, gx_got[c]):
                gx = put(gx, got, bits, c * step)
        gains = gains + to_peer(gains, 1)
        gains = lax.dynamic_slice_in_dim(gains, me * (d_model // n_sp), d_model // n_sp, axis=1)
        total = lambda terms: terms[0] + terms[1] + terms[2]
        join = lambda arr: arr.reshape(x_loc.shape)
        return (join(y), join(gx), gains[0], *map(total, sums), gains[1], gains[2])

    seq_spec = P('dp', 'sp', None)
    mat_rep = P(None, None)
    vec_rep = P(None)
    row_spec = P(('dp', 'sp'), None)
    vec_spec = P(('dp', 'sp'))
    return jax.shard_map(device_step, mesh=mesh, in_specs=(seq_spec, seq_spec, P('dp', 'sp'), vec_rep, mat_rep, mat_rep, mat_rep, mat_rep, vec_rep, vec_rep), out_specs=(seq_spec, seq_spec, vec_spec, row_spec, row_spec, row_spec, row_spec, vec_spec, vec_spec), check_vma=False)
```

```python
import math
import jax
import jax.numpy as jnp
from jax import lax
from jax.experimental import pallas as pl
from jax.experimental.pallas import tpu as pltpu
from jax.sharding import PartitionSpec as P


HEAD = 128
EPS = 1e-5
ROPE_BASE = 10000.0
NEG_BIG = -1e30
SCALE = HEAD ** -0.5
SCALE2 = SCALE * math.log2(math.e)
N_CHUNK = 2
VMEM = 66_000_000
F32 = jnp.float32
BF16 = jnp.bfloat16


def dot_nn(a, b):
    return lax.dot_general(a, b, (((1,), (0,)), ((), ())), preferred_element_type=F32)


def dot_nt(a, b):
    return lax.dot_general(a, b, (((1,), (1,)), ((), ())), preferred_element_type=F32)


def dot_tn(a, b):
    return lax.dot_general(a, b, (((0,), (0,)), ((), ())), preferred_element_type=F32)


def head_cols(idx):
    return slice(idx * HEAD, (idx + 1) * HEAD)


def row_sum(part):
    return jnp.sum(part, axis=-1, keepdims=True)


ANY = pl.BlockSpec(memory_space=pl.ANY)


def place(bits):
    return 3 - bits


def front_own_kernel(*refs):
    dy_ref, *dy_outs = refs[11], *refs[-N_CHUNK:]
    per = pl.num_programs(1) // N_CHUNK
    for c, out_ref in enumerate(dy_outs):
        @pl.when((pl.program_id(0) == 0) & (pl.program_id(1) // per == c))
        def _():
            out_ref[...] = dy_ref[...]

    front_kernel(*refs[:11], *refs[12:-N_CHUNK])


def front_kernel(me_ref, xa_ref, xb_ref, cos_ref, sin_ref, gn_ref, gq_ref, gk_ref, wq_ref, wk_ref, wv_ref, *refs):
    x_ref, h_ref, q_ref, k_ref, v_ref, q1_ref, k1_ref = refs[-7:]
    d_model = x_ref.shape[-1]
    n_heads = d_model // HEAD

    @pl.when(pl.program_id(0) == 0)
    def _():
        x_ref[...] = xa_ref[...]

    @pl.when(pl.program_id(0) == 1)
    def _():
        x_ref[...] = xb_ref[...]

    x_f = x_ref[...].astype(F32)
    inv_x = lax.rsqrt(jnp.mean(x_f * x_f, axis=-1, keepdims=True) + EPS)
    hidden = (x_f * inv_x * gn_ref[...]).astype(BF16)
    blk = d_model // 4
    for b in range(4):
        h_ref[:, pl.ds(pl.multiple_of(place(me_ref[0] ^ b) * blk, blk), blk)] = hidden[:, b * blk:(b + 1) * blk]
    cos_t = cos_ref[...]
    sin_t = sin_ref[...]
    n_col = 512
    for w_ref, g_ref, raw_ref, out_ref in ((wq_ref, gq_ref, q1_ref, q_ref), (wk_ref, gk_ref, k1_ref, k_ref)):
        sq = jnp.zeros((x_ref.shape[0], HEAD), F32)
        for c0 in range(0, d_model, n_col):
            raw = dot_nn(hidden, w_ref[:, c0:c0 + n_col])
            raw_ref[:, c0:c0 + n_col] = raw
            for j in range(n_col // HEAD):
                piece = raw[:, head_cols(j)]
                sq = sq + piece * piece
        inv = lax.rsqrt(row_sum(sq) * (1.0 / d_model) + EPS)
        for j in range(n_heads):
            u = raw_ref[:, head_cols(j)] * inv * g_ref[:, head_cols(j)]
            rot = u * cos_t + pltpu.roll(u, HEAD // 2, 1) * sin_t
            out_ref[:, head_cols(j)] = rot.astype(BF16)
    for c0 in range(0, d_model, n_col):
        v_ref[:, c0:c0 + n_col] = dot_nn(hidden, wv_ref[:, c0:c0 + n_col]).astype(BF16)


def front(me, x_a, x_b, own, bits, seq0, n_seq, cos_t, sin_t, g_norm, g_query, g_key, w_query, w_key, w_value, filled, grad_y=None):
    n_piece, n_all, rows, d_model = cos_t.shape[:3] + x_a.shape[-1:]
    first = lambda i, s: jnp.where(i == 0, s, n_seq - 1)
    second = lambda i, s: jnp.where(i == 0, 0, s)
    x_block = (None, rows, d_model)
    a_map = (lambda i, s, m: (m[0] * n_all + first(i, s), 0, 0)) if own else (lambda i, s, m: (first(i, s), 0, 0))
    spot = lambda i, s, m: (m[0] ^ jnp.where(i == 0, bits[0], bits[1]), seq0 + s, 0, 0)
    table = pl.BlockSpec((None, None, rows, HEAD), spot)
    out = pl.BlockSpec((None, None, rows, d_model), spot)
    vec = pl.BlockSpec((1, d_model), lambda i, s, m: (0, 0))
    mat = pl.BlockSpec((d_model, d_model), lambda i, s, m: (0, 0), pipeline_mode=pl.Buffered(1))
    big = lambda dt: jax.ShapeDtypeStruct((n_piece, n_all, rows, d_model), dt)
    row = lambda g: g.astype(F32).reshape(1, d_model)
    n_tok = 2 * n_seq * rows
    per = n_seq // N_CHUNK

    def own_out(c):
        return pl.BlockSpec((None, None, rows, d_model), lambda i, s, m: (m[0], jnp.clip(first(i, s) - c * per, 0, per - 1), 0, 0))

    dy_in, dy_outs, dy_shapes = [], [], []
    if own:
        dy_in = [pl.BlockSpec(x_block, a_map)]
        dy_outs = [own_out(c) for c in range(N_CHUNK)]
        dy_shapes = [jax.ShapeDtypeStruct((n_piece, per, rows, d_model), BF16)] * N_CHUNK
    return pl.pallas_call(
        front_own_kernel if own else front_kernel,
        grid_spec=pltpu.PrefetchScalarGridSpec(
            num_scalar_prefetch=1,
            grid=(2, n_seq),
            in_specs=[pl.BlockSpec(x_block, a_map), pl.BlockSpec(x_block, lambda i, s, m: (second(i, s), 0, 0)), table, table, vec, vec, vec, mat, mat, mat] + dy_in + [ANY] * len(filled),
            out_specs=[out] * 7 + dy_outs,
        ),
        out_shape=[big(BF16)] * 5 + [big(F32)] * 2 + dy_shapes,
        input_output_aliases={11 + n: n for n in range(len(filled))},
        compiler_params=pltpu.CompilerParams(vmem_limit_bytes=VMEM, dimension_semantics=("arbitrary", "arbitrary")),
        cost_estimate=pl.CostEstimate(flops=6 * n_tok * d_model * d_model, bytes_accessed=n_tok * d_model * 20 + 6 * d_model * d_model, transcendentals=0),
        name="front",
    )(me, x_a, x_b, cos_t, sin_t, row(g_norm), row(g_query), row(g_key), w_query, w_key, w_value, *([grad_y] if own else []), *filled)


def attend_kernel(me_ref, q_ref, k_ref, v_ref, *refs):
    rel_ref, o_ref, lse_ref = refs[-3:]
    n_piece, _, rows, width = q_ref.shape
    keep = lax.broadcasted_iota(jnp.int32, (rows, rows), 0) <= lax.broadcasted_iota(jnp.int32, (rows, rows), 1)
    for hd in range(width // HEAD):
        cols = head_cols(hd)
        v_t = [v_ref[j, 0, :, cols].T for j in range(n_piece)]
        for i in range(n_piece):
            q_i = q_ref[i, 0, :, cols]
            scores = [dot_nt(k_ref[j, 0, :, cols], q_i) for j in range(i + 1)]
            scores[i] = jnp.where(keep, scores[i], NEG_BIG)
            top = scores[0]
            for j in range(1, i + 1):
                top = jnp.maximum(top, scores[j])
            top = jnp.max(top, axis=0, keepdims=True) * SCALE2
            total = None
            out = None
            for j in range(i + 1):
                prob = jnp.exp2(scores[j] * SCALE2 - top)
                part = jnp.sum(prob, axis=0, keepdims=True)
                total = part if total is None else total + part
                term = dot_nn(v_t[j], prob.astype(BF16))
                out = term if out is None else out + term
            out = (out * (1.0 / total)).astype(BF16).T
            o_ref[i, 0, :, cols] = out
            rel_ref[i, 0, :, cols] = out
            lse_ref[0, hd, :, i * rows:(i + 1) * rows] = top + jnp.log2(total)


def attend(me, q_all, k_all, v_all, seq0, n_seq, filled, heads=2):
    n_piece, n_all, rows, d_model = q_all.shape
    n_heads = d_model // HEAD
    per = n_heads // heads // 4
    shape = (n_piece, 1, rows, heads * HEAD)
    blk = pl.BlockSpec(shape, lambda s, h, m: (0, seq0 + s, 0, h))
    rel = pl.BlockSpec(shape, lambda s, h, m: (0, s, 0, place(m[0] ^ (h // per)) * per + h % per))
    seq = n_piece * rows
    big = jax.ShapeDtypeStruct(q_all.shape, BF16)
    return pl.pallas_call(
        attend_kernel,
        grid_spec=pltpu.PrefetchScalarGridSpec(
            num_scalar_prefetch=1,
            grid=(n_seq, n_heads // heads),
            in_specs=[blk] * 3 + [ANY] * len(filled),
            out_specs=[rel, blk, pl.BlockSpec((1, heads, 1, seq), lambda s, h, m: (seq0 + s, h, 0, 0))],
        ),
        out_shape=[jax.ShapeDtypeStruct((n_piece, n_seq, rows, d_model), BF16), big, jax.ShapeDtypeStruct((n_all, n_heads, 1, seq), F32)],
        input_output_aliases={4 + n: n + 1 for n in range(len(filled))},
        compiler_params=pltpu.CompilerParams(vmem_limit_bytes=VMEM, dimension_semantics=("arbitrary", "arbitrary")),
        cost_estimate=pl.CostEstimate(flops=6 * n_seq * seq * seq * d_model, bytes_accessed=10 * n_seq * seq * d_model, transcendentals=0),
        name="attend",
    )(me, q_all, k_all, v_all, *filled)


def attend_back_kernel(q_ref, k_ref, v_ref, do_ref, lse_ref, *refs):
    dq_ref, dk_ref, dv_ref, dk_acc, dv_acc = refs[-5:]
    n_piece, _, rows, width = q_ref.shape
    keep = lax.broadcasted_iota(jnp.int32, (rows, rows), 0) <= lax.broadcasted_iota(jnp.int32, (rows, rows), 1)
    for hd in range(width // HEAD):
        cols = head_cols(hd)
        k_t = [k_ref[j, 0, :, cols].T for j in range(n_piece)]
        for i in range(n_piece):
            q_i = q_ref[i, 0, :, cols]
            do_i = do_ref[i, 0, :, cols]
            lse = lse_ref[0, hd, :, i * rows:(i + 1) * rows]
            probs, d_probs = [], []
            row_dot = None
            for j in range(i + 1):
                prob = jnp.exp2(dot_nt(k_ref[j, 0, :, cols], q_i) * SCALE2 - lse)
                if j == i:
                    prob = jnp.where(keep, prob, 0.0)
                d_prob = dot_nt(v_ref[j, 0, :, cols], do_i)
                part = jnp.sum(prob * d_prob, axis=0, keepdims=True)
                row_dot = part if row_dot is None else row_dot + part
                probs.append(prob)
                d_probs.append(d_prob)
            dq_t = None
            for j in range(i + 1):
                d_s = (probs[j] * (d_probs[j] - row_dot)).astype(BF16)
                dv_term = dot_nn(probs[j].astype(BF16), do_i)
                dk_term = dot_nn(d_s, q_i)
                dq_term = dot_nn(k_t[j], d_s)
                dq_t = dq_term if dq_t is None else dq_t + dq_term
                if i == j:
                    dv_acc[hd, j] = dv_term
                    dk_acc[hd, j] = dk_term
                else:
                    dv_acc[hd, j] += dv_term
                    dk_acc[hd, j] += dk_term
            dq_ref[i, 0, :, cols] = (dq_t * SCALE).astype(BF16).T
        for j in range(n_piece):
            dk_ref[j, 0, :, cols] = (dk_acc[hd, j] * SCALE).astype(BF16)
            dv_ref[j, 0, :, cols] = dv_acc[hd, j].astype(BF16)


def attend_back(q_all, k_all, v_all, d_out, lse, seq0, n_seq, filled, heads=2):
    n_piece, _, rows, d_model = q_all.shape
    n_heads = d_model // HEAD
    shape = (n_piece, 1, rows, heads * HEAD)
    blk = pl.BlockSpec(shape, lambda s, h: (0, seq0 + s, 0, h))
    loc = pl.BlockSpec(shape, lambda s, h: (0, s, 0, h))
    seq = n_piece * rows
    return pl.pallas_call(
        attend_back_kernel,
        grid=(n_seq, n_heads // heads),
        in_specs=[blk] * 3 + [loc, pl.BlockSpec((1, heads, 1, seq), lambda s, h: (seq0 + s, h, 0, 0))] + [ANY] * len(filled),
        out_specs=[loc, loc, blk],
        out_shape=[jax.ShapeDtypeStruct(d_out.shape, BF16)] * 2 + [jax.ShapeDtypeStruct(q_all.shape, BF16)],
        input_output_aliases={5: 2} if filled else {},
        scratch_shapes=[pltpu.VMEM((heads, n_piece, rows, HEAD), F32)] * 2,
        compiler_params=pltpu.CompilerParams(vmem_limit_bytes=VMEM, dimension_semantics=("arbitrary", "arbitrary")),
        cost_estimate=pl.CostEstimate(flops=14 * n_seq * seq * seq * d_model, bytes_accessed=14 * n_seq * seq * d_model, transcendentals=0),
        name="attend_back",
    )(q_all, k_all, v_all, d_out, lse, *filled)


def tail_kernel(dq_ref, dk_ref, dv_ref, q1_ref, k1_ref, x_ref, dy_ref, cos_ref, sin_ref, gn_ref, gq_ref, gk_ref, wq_ref, wk_ref, wv_ref, *refs):
    dqr_ref, dkr_ref, gx_ref, ggn_ref, ggq_ref, ggk_ref, dh_ref, rot_ref = refs[-8:]
    rows, d_model = x_ref.shape
    n_heads = d_model // HEAD
    n_col = 512
    cos_t = cos_ref[...]
    sin_t = sin_ref[...]

    @pl.when((pl.program_id(0) == 0) & (pl.program_id(1) == 0))
    def _():
        for ref in (ggn_ref, ggq_ref, ggk_ref):
            ref[...] = jnp.zeros_like(ref)

    dv_b = dv_ref[...]
    for c0 in range(0, d_model, n_col):
        dh_ref[:, c0:c0 + n_col] = dot_nt(dv_b, wv_ref[c0:c0 + n_col, :])
    for d_ref, raw_ref, g_ref, w_ref, dr_ref, gg_ref in ((dq_ref, q1_ref, gq_ref, wq_ref, dqr_ref, ggq_ref), (dk_ref, k1_ref, gk_ref, wk_ref, dkr_ref, ggk_ref)):
        sq = jnp.zeros((rows, HEAD), F32)
        cross = jnp.zeros((rows, HEAD), F32)
        for j in range(n_heads):
            u = raw_ref[:, head_cols(j)]
            d = d_ref[:, head_cols(j)].astype(F32)
            d = d * cos_t - pltpu.roll(d, HEAD // 2, 1) * sin_t
            rot_ref[:, head_cols(j)] = d
            sq = sq + u * u
            cross = cross + d * g_ref[:, head_cols(j)] * u
        inv = lax.rsqrt(row_sum(sq) * (1.0 / d_model) + EPS)
        coef = row_sum(cross) * (1.0 / d_model) * inv * inv
        for j in range(n_heads):
            u = raw_ref[:, head_cols(j)]
            d = rot_ref[:, head_cols(j)]
            gg_ref[:, head_cols(j)] += jnp.sum(d * (u * inv), axis=0, keepdims=True)
            dr_ref[:, head_cols(j)] = (inv * (d * g_ref[:, head_cols(j)] - u * coef)).astype(BF16)
        d_b = dr_ref[...]
        for c0 in range(0, d_model, n_col):
            dh_ref[:, c0:c0 + n_col] += dot_nt(d_b, w_ref[c0:c0 + n_col, :])
    sq = jnp.zeros((rows, HEAD), F32)
    cross = jnp.zeros((rows, HEAD), F32)
    for j in range(n_heads):
        u = x_ref[:, head_cols(j)].astype(F32)
        sq = sq + u * u
        cross = cross + dh_ref[:, head_cols(j)] * gn_ref[:, head_cols(j)] * u
    inv = lax.rsqrt(row_sum(sq) * (1.0 / d_model) + EPS)
    coef = row_sum(cross) * (1.0 / d_model) * inv * inv
    for j in range(n_heads):
        u = x_ref[:, head_cols(j)].astype(F32)
        d = dh_ref[:, head_cols(j)]
        ggn_ref[:, head_cols(j)] += jnp.sum(d * (u * inv), axis=0, keepdims=True)
        g_x = dy_ref[:, head_cols(j)].astype(F32) + inv * (d * gn_ref[:, head_cols(j)] - u * coef)
        gx_ref[:, head_cols(j)] = g_x.astype(BF16)


def tail(dq, dk, dv, q1, k1, x_all, dy, cos_t, sin_t, g_norm, g_query, g_key, w_query, w_key, w_value, seq0, n_seq, filled):
    n_piece, _, rows, d_model = x_all.shape
    spot = lambda i, s: (i, seq0 + s, 0, 0)
    tok = pl.BlockSpec((None, None, rows, d_model), spot)
    loc = pl.BlockSpec((None, None, rows, d_model), lambda i, s: (i, s, 0, 0))
    table = pl.BlockSpec((None, None, rows, HEAD), spot)
    vec = pl.BlockSpec((1, d_model), lambda i, s: (0, 0))
    mat = pl.BlockSpec((d_model, d_model), lambda i, s: (0, 0), pipeline_mode=pl.Buffered(1))
    big = jax.ShapeDtypeStruct(x_all.shape, BF16)
    small = jax.ShapeDtypeStruct((1, d_model), F32)
    row = lambda g: g.astype(F32).reshape(1, d_model)
    n_tok = n_piece * n_seq * rows
    return pl.pallas_call(
        tail_kernel,
        grid=(n_piece, n_seq),
        in_specs=[loc] * 2 + [tok] * 4 + [loc] + [table] * 2 + [vec] * 3 + [mat] * 3 + [ANY] * len(filled),
        out_specs=[tok] * 3 + [vec] * 3,
        out_shape=[big] * 3 + [small] * 3,
        input_output_aliases={15 + n: n for n in range(len(filled))},
        scratch_shapes=[pltpu.VMEM((rows, d_model), F32)] * 2,
        compiler_params=pltpu.CompilerParams(vmem_limit_bytes=VMEM, dimension_semantics=("arbitrary", "arbitrary")),
        cost_estimate=pl.CostEstimate(flops=6 * n_tok * d_model * d_model, bytes_accessed=n_tok * d_model * 24 + 6 * d_model * d_model, transcendentals=0),
        name="tail",
    )(dq, dk, dv, q1, k1, x_all, dy, cos_t, sin_t, row(g_norm), row(g_query), row(g_key), w_query, w_key, w_value, *filled)


def rope_tables(positions):
    half = HEAD // 2
    inv_freq = ROPE_BASE ** (-jnp.arange(half, dtype=F32) * (2.0 / HEAD))
    angles = positions.astype(F32)[..., None] * inv_freq
    cos_t = jnp.cos(angles)
    sin_t = jnp.sin(angles)
    return jnp.concatenate([cos_t, cos_t], axis=-1), jnp.concatenate([-sin_t, sin_t], axis=-1)


def after(value, *earlier):
    return lax.optimization_barrier((value,) + earlier)[0]


def solution(mesh):
    n_sp = mesh.shape['sp']

    def to_peer(value, bits):
        return lax.ppermute(value, 'sp', [(i, i ^ bits) for i in range(n_sp)])

    def device_step(x_loc, grad_y, positions, g_norm, w_query, w_key, w_value, w_out, g_query, g_key):
        n_batch, rows, d_model = x_loc.shape
        n_seq = n_batch // n_sp
        step = n_seq // N_CHUNK
        me = lax.axis_index('sp')
        me_vec = jnp.reshape(me, (1,)).astype(jnp.int32)
        shape4 = (n_sp, n_seq, rows, d_model)
        flat = lambda arr: arr.reshape(-1, d_model)
        far_bits = (2, 3, 1)

        def piece(arr, bits, seq0, count):
            return lax.dynamic_slice(arr, (me ^ bits, seq0, 0, 0), (1, count, rows, d_model))

        def pieces(arr, seq0, count):
            cut = lax.optimization_barrier((arr,) + tuple(piece(arr, bits, seq0, count) for bits in far_bits))
            return cut[0], cut[1:]

        def send(parts):
            return [to_peer(p, bits) for p, bits in zip(parts, far_bits)]

        def put(buf, got, bits, seq0):
            return lax.dynamic_update_slice(buf, got, (me ^ bits, seq0, 0, 0))

        def grad_rows(rels, rights):
            blk = d_model // n_sp

            def part(n, grads):
                terms = [dot_tn(flat(r)[:, n * blk:(n + 1) * blk], flat(g)) for r, g in zip(rels, grads)]
                return sum(terms[1:], terms[0])

            given = to_peer(part(0, rights), 1)
            far = lax.optimization_barrier(part(1, rights)) + given
            got = to_peer(far, 2)

            def rest(prev):
                late = [after(g, prev) for g in rights]
                given = to_peer(part(2, late), 1)
                mine = lax.optimization_barrier(part(3, late))
                return lax.optimization_barrier(mine + given), got

            return rest, far

        pos4 = positions.reshape(n_sp, n_seq, rows)
        pos4, *cut = lax.optimization_barrier([pos4] + [lax.dynamic_slice_in_dim(pos4, me ^ bits, 1, axis=0) for bits in far_bits])
        for bits, got in zip(far_bits, send(cut)):
            pos4 = lax.dynamic_update_slice_in_dim(pos4, got, me ^ bits, axis=0)
        x4 = x_loc.reshape(shape4)
        x_parts = []
        for c in range(N_CHUNK):
            x_parts.append([])
            for bits in (2, 3):
                x_parts[-1].append(piece(x4, bits, c * step, step)[0])
                x4 = after(x4, *x_parts[-1])
            if c == 0:
                x_near = piece(x4, 1, 0, n_seq)[0]
                x4 = after(x4, x_near)
        x_far = [[to_peer(p, bits) for p, bits in zip(x_parts[c], (2, 3))] for c in range(N_CHUNK)]
        dy4 = after(grad_y.reshape(shape4), *x_parts[1])
        x_near = to_peer(x_near, 1)
        dy_got = [send([piece(dy4, bits, c * step, step) for bits in far_bits]) for c in range(N_CHUNK)]
        cos_t, sin_t = rope_tables(pos4)
        gains_in = (g_norm, g_query, g_key)
        weights = (w_query, w_key, w_value)
        filled = front(me_vec, x_loc, x_near, True, (0, 1), 0, n_seq, cos_t, sin_t, *gains_in, *weights, (), grad_y)
        filled, dys = filled[:7], list(filled[7:])
        attn = ()
        rels = []
        prev = cos_t
        for c in range(N_CHUNK):
            filled = front(me_vec, x_far[c][0], x_far[c][1], False, (2, 3), c * step, step, after(cos_t, prev), sin_t, *gains_in, *weights, tuple(filled))
            rel, *attn = attend(me_vec, filled[2], filled[3], filled[4], c * step, step, tuple(attn))
            rels.append(rel)
            prev = attn[1]
        x_all, h_rel, q, k, v, q1, k1 = filled
        attn, lse = attn
        y = (flat(x_all).astype(F32) + dot_nn(flat(attn), w_out)).astype(BF16).reshape(shape4)
        y, y_parts = pieces(y, 0, n_seq)
        y_got = send(y_parts)
        prev = y_parts[0]
        dv, tails, gx_got, dqk = (), (), [], []
        for c in range(N_CHUNK):
            dy = dys[c]
            for bits, got in zip(far_bits, dy_got[c]):
                dy = put(dy, after(got, prev), bits, 0)
            dys[c] = dy
            if c == N_CHUNK - 1:
                w_o, prev = grad_rows(rels, dys)
            d_attn = dot_nt(flat(dy), w_out).astype(BF16).reshape(dy.shape)
            dq, dk, *dv = attend_back(q, k, v, d_attn, after(lse, prev), c * step, step, tuple(dv))
            dqk.append((dq, dk))
            prev = dq
        w_v, prev = grad_rows([h_rel], dv)
        gains = 0.0
        for c in range(N_CHUNK):
            *tails, ggn, ggq, ggk = tail(*dqk[c], dv[0], q1, k1, x_all, dys[c], after(cos_t, prev), sin_t, *gains_in, *weights, c * step, step, tuple(tails))
            gains = gains + jnp.concatenate([ggn, ggq, ggk], axis=0)
            tails[2], gx_parts = pieces(tails[2], c * step, step)
            if c == N_CHUNK - 1:
                gains = gains + to_peer(gains, 2)
            gx_got.append(send(gx_parts))
            prev = gx_parts[0]
        dqr, dkr, gx = tails
        w_q, prev = grad_rows([h_rel], [after(dqr, prev)])
        w_k, prev = grad_rows([h_rel], [after(dkr, prev)])
        sums = []
        for rest in (w_q, w_k, w_v, w_o):
            sums.append(rest(prev))
            prev = sums[-1][0]
        g_wq, g_wv, g_wo = (sums[n][0] + sums[n][1] for n in (0, 2, 3))
        g_wk = after(sums[1][0], g_wq, g_wv, g_wo) + sums[1][1]
        for bits, got in zip(far_bits, y_got):
            y = put(y, after(got, prev), bits, 0)
        for c in range(N_CHUNK):
            for bits, got in zip(far_bits, gx_got[c]):
                gx = put(gx, got, bits, c * step)
        gains = gains + to_peer(gains, 1)
        gains = lax.dynamic_slice_in_dim(gains, me * (d_model // n_sp), d_model // n_sp, axis=1)
        join = lambda arr: arr.reshape(x_loc.shape)
        return (join(y), join(gx), gains[0], g_wq, g_wk, g_wv, g_wo, gains[1], gains[2])

    seq_spec = P('dp', 'sp', None)
    mat_rep = P(None, None)
    vec_rep = P(None)
    row_spec = P(('dp', 'sp'), None)
    vec_spec = P(('dp', 'sp'))
    return jax.shard_map(device_step, mesh=mesh, in_specs=(seq_spec, seq_spec, P('dp', 'sp'), vec_rep, mat_rep, mat_rep, mat_rep, mat_rep, vec_rep, vec_rep), out_specs=(seq_spec, seq_spec, vec_spec, row_spec, row_spec, row_spec, row_spec, vec_spec, vec_spec), check_vma=False)
```
